32 devices in a mesh: layer: 4 (over y, x), row: 2 (over core), col: 4 (over z).
Axes of the slice: x: 2, y: 2, z: 4, core: 2. Of those that a mesh axis runs over, the one named last changes fastest.
Arguments:
- block_values: bfloat16 [4, 2, 4, 32, 256, 256], P('layer', 'row', 'col'), may hold values from 0 to 3
- block_rows: int32 [4, 2, 4, 32], P('layer', 'row', 'col'), may hold values from 0 to 255
- block_cols: int32 [4, 2, 4, 32], P('layer', 'row', 'col'), may hold values from 0 to 127
- block_count: int32 [4, 2, 4], P('layer', 'row', 'col'), may hold values from 1 to 32, as said below
- dangling: int32 [4, 2, 4, 16384], P('layer', 'row', 'col'), may hold values 0 or 1
- start_ranks: float32 [4, 2, 4, 16384], P('layer', 'row', 'col'), may hold values from 0.2 to 5
Outputs:
- ranks: float32 [4, 2, 4, 16384], P('layer', 'row', 'col')
- residuals: float32 [3, 4], P(None, 'layer')
The draws below stay inside these ranges and needn't reach their ends.
Inputs may be any that keep to these rules, and one draw needn't show every extreme that they name: `block_count`: live slots of a tile; in every layer some tile has all 32 slots live. `block_rows`: slots at or past a tile's count carry no edges; coordinates may repeat within a tile, and repeated blocks add.
All inputs are finite; a program needn't handle non-finite values. No bound on the sum of `dangling` on one device may be relied on, other than what follows from the above.
Results may differ from the reference program's by a relative error of at most 0.0012.
Values may be sent and summed in bfloat16 or wider, within the bound.
No kernel may reach another device: no remote copies, remote signals or barrier semaphores. Data moves between devices by JAX's collectives and lax.ppermute only.
A program may use at most 64 MiB of HBM per device.

```python
import math
import jax
import jax.numpy as jnp
from jax import lax

BLOCK = 256
MAXB = 32
ITERS = 3
ROW_BLK = 256
LAYERS = 4
NODES = 131072
SPAN = 16384
COL_BLK = 128
N_ROW = 2
N_COL = 4


def draw_block_values(key, part):
    shape = (LAYERS, N_ROW, N_COL, MAXB, BLOCK, BLOCK)
    first_key = jax.random.fold_in(jax.random.fold_in(key, 11), 0)
    values = jnp.exp(jax.random.uniform(first_key, shape, jnp.float32, math.log(0.05), 0.0))
    return values.astype(jnp.bfloat16)


def draw_block_count(key, part):
    first_key, second_key = jax.random.split(jax.random.fold_in(key, 23))
    tiles = N_ROW * N_COL
    counts = jax.random.randint(first_key, (LAYERS, tiles), max(1, MAXB // 4), MAXB + 1, jnp.int32)
    fullest = jax.random.randint(second_key, (LAYERS, 1), 0, tiles, jnp.int32)
    counts = jnp.where(jnp.arange(tiles, dtype=jnp.int32)[None, :] == fullest, MAXB, counts)
    return counts.reshape(LAYERS, N_ROW, N_COL).astype(jnp.int32)


def touch_ends(values, rng, low, largest):
    dims = values.shape
    index_at = [jax.random.randint(jax.random.fold_in(rng, axis), (), 0, dims[axis]) for axis in range(len(dims))]
    values = values.at[tuple(index_at)].set(low)
    longest = dims.index(max(dims))
    index_at[longest] = (index_at[longest] + 1) % dims[longest]
    return values.at[tuple(index_at)].set(largest)


def steps_of(rng, dims, cuts, smallest, largest):
    level, own = 1.0, jax.random.fold_in(rng, 6)
    for axis_at, parts in cuts:
        draws = jnp.exp(jax.random.uniform(jax.random.fold_in(own, axis_at), (parts,), jnp.float32, smallest / len(cuts), largest / len(cuts)))
        level = level * jnp.repeat(draws, dims[axis_at] // parts).reshape([-1 if axis == axis_at else 1 for axis in range(len(dims))])
    return level


def setup_inputs(seed: int = 0) -> dict:
    arg_keys = jax.random.split(jax.random.key(seed), 7)
    return {
        "block_values": draw_block_values(jax.random.fold_in(arg_keys[6], 71), 0),
        "block_rows": touch_ends(jax.random.randint(arg_keys[1], (LAYERS, N_ROW, N_COL, MAXB), 0, ROW_BLK), jax.random.fold_in(arg_keys[1], 1), 0, ROW_BLK - 1).astype(jnp.int32),
        "block_cols": touch_ends(jax.random.randint(arg_keys[2], (LAYERS, N_ROW, N_COL, MAXB), 0, COL_BLK), jax.random.fold_in(arg_keys[2], 1), 0, COL_BLK - 1).astype(jnp.int32),
        "block_count": draw_block_count(jax.random.fold_in(arg_keys[6], 71), 0),
        "dangling": touch_ends((jax.random.randint(arg_keys[4], (LAYERS, N_ROW, N_COL, SPAN), 0, 8) < 1).astype(jnp.int32), jax.random.fold_in(arg_keys[4], 1), 0, 1),
        "start_ranks": jnp.clip(jnp.exp(math.log(5.0) - 3.218876 * jax.random.uniform(arg_keys[5], (LAYERS, N_ROW, N_COL, SPAN), jnp.float32) ** steps_of(arg_keys[5], (LAYERS, N_ROW, N_COL, SPAN), ((0, 4), (1, 2), (2, 4)), -0.2, 0.2)), 0.2, 5.0),
    }


damping = 0.85
coupling = 0.3


def reference(block_values, block_rows, block_cols, block_count, dangling, start_ranks):
    live_slot = (jnp.arange(MAXB)[None, None, None, :] < block_count[..., None]).astype(jnp.float32)

    def degree_layer(packed):
        values, cols_here, live_here = packed
        colsum = jnp.einsum('rcsij->rcsj', values.astype(jnp.float32))
        onehot = (cols_here[..., None] == jnp.arange(COL_BLK)[None, None, None, :]).astype(jnp.float32) * live_here[..., None]
        deg_group = jnp.einsum('rcsb,rcsj->cbj', onehot, colsum, precision=lax.Precision.HIGHEST)
        return jnp.transpose(deg_group.reshape(N_COL, N_ROW, SPAN), (1, 0, 2))

    degree = lax.map(degree_layer, (block_values, block_cols, live_slot))
    keep_mask = 1.0 - dangling.astype(jnp.float32)
    denominator = keep_mask * degree + 1.0
    layer_ids = jnp.arange(LAYERS)
    spread = jnp.where((layer_ids == 0) | (layer_ids == LAYERS - 1), 1.0, 0.5).astype(jnp.float32) * coupling
    spread = spread.reshape(LAYERS, 1, 1, 1)

    def walk_layer(packed):
        values, rows_here, cols_here, live_here, scaled_here = packed
        column_bf = jnp.transpose(scaled_here, (1, 0, 2)).reshape(N_COL, COL_BLK, BLOCK)
        picked = column_bf[jnp.arange(N_COL)[None, :, None], cols_here]
        products = jnp.einsum('rcsij,rcsj->rcsi', values.astype(jnp.float32), picked.astype(jnp.float32))
        onehot = (rows_here[..., None] == jnp.arange(ROW_BLK)[None, None, None, :]).astype(jnp.float32) * live_here[..., None]
        walk_sum = jnp.einsum('rcsb,rcsi->rbi', onehot, products, precision=lax.Precision.HIGHEST)
        return walk_sum.reshape(N_ROW, N_COL, SPAN)

    ranks_now = start_ranks
    residual_list = []
    for iteration in range(ITERS):
        scaled = (ranks_now * keep_mask / denominator).astype(jnp.bfloat16)
        walk_sum = lax.map(walk_layer, (block_values, block_rows, block_cols, live_slot, scaled))
        dangle_mass = jnp.sum(ranks_now / denominator, axis=(1, 2, 3), keepdims=True)
        spill = ranks_now * spread
        padded = jnp.pad(spill, ((1, 1), (0, 0), (0, 0), (0, 0)))
        arrive = padded[:-2] + padded[2:]
        updated = damping * ((1.0 - coupling) * (walk_sum + dangle_mass / NODES) + arrive) + (1.0 - damping)
        residual_list.append(jnp.sum(jnp.abs(updated - ranks_now), axis=(1, 2, 3)))
        ranks_now = updated
    return ranks_now, jnp.stack(residual_list)
```

```python
import functools
import jax
import jax.numpy as jnp
from jax import lax
from jax.experimental import pallas as pl
from jax.experimental.pallas import tpu as pltpu
from jax.sharding import PartitionSpec as P

ITERS = 3
damping = 0.85
coupling = 0.3

F32 = jnp.float32
BF16 = jnp.bfloat16
VMEM = pl.BlockSpec(memory_space=pltpu.VMEM)
SMEM = pl.BlockSpec(memory_space=pltpu.SMEM)
META = 8


def call(body, name, outs, specs, scratch=()):
    return pl.pallas_call(
        body,
        name=name,
        out_shape=outs,
        in_specs=specs,
        out_specs=jax.tree.map(lambda _: VMEM, outs),
        scratch_shapes=scratch,
        compiler_params=pltpu.CompilerParams(vmem_limit_bytes=24 * 1024 * 1024),
    )


def two_terms(x):
    hi = x.astype(BF16)
    return hi, (x - hi.astype(F32)).astype(BF16)


def place(onehot, rows):
    hi, lo = two_terms(rows)
    return jnp.dot(onehot, hi, preferred_element_type=F32) + jnp.dot(
        onehot, lo, preferred_element_type=F32
    )


def to_blocks(ref, edge):
    wide = edge // 128
    count = ref.shape[0] // wide
    return jnp.concatenate([ref[pl.ds(w, count, wide), :] for w in range(wide)], axis=1)


def opening(values, cols, count, x, dangling, out):
    slots, edge, _ = values.shape
    blocks = x.shape[0] * 128 // edge
    ones = jnp.ones((16, edge), BF16)
    for s in range(slots):
        out[s : s + 1, :] = jnp.dot(ones, values[s], preferred_element_type=F32)[0:1, :]
    out[slots : slots + META, :] = jnp.zeros((META, edge), F32)
    slot_ids = lax.broadcasted_iota(jnp.int32, (1, slots), 1)
    out[slots : slots + 1, 0:slots] = jnp.where(slot_ids < count[0], cols[...], -1).astype(F32)
    at = slots + META
    out[at : at + blocks, :] = to_blocks(x, edge)
    out[at + blocks : at + 2 * blocks, :] = 1.0 - to_blocks(dangling, edge).astype(F32)


def products(values, cols_s, scaled, picked, payload):
    slots = values.shape[0]
    for s in range(slots):
        picked[s : s + 1, :] = scaled[pl.ds(cols_s[s], 1), :]
    group = 16
    for g in range(slots // group):
        lhs = picked[g * group : (g + 1) * group, :].astype(BF16)
        for k in range(group):
            s = g * group + k
            got = lax.dot_general(
                lhs, values[s], (((1,), (1,)), ((), ())), preferred_element_type=F32
            )
            payload[s : s + 1, :] = got[k : k + 1, :]


def send_out(ids, layers, pair_rows, x, inv, kinv, rows, count, payload, spill, scaled, xcur):
    slots = rows.shape[1]
    edge = x.shape[1]
    scaled[...] = (x * kinv).astype(BF16).astype(F32)
    layer = ids[0]
    spread = jnp.where((layer == 0) | (layer == layers - 1), 1.0, 0.5).astype(F32) * coupling
    if x.shape[0] == pair_rows:
        own = x
    else:
        own = xcur[pl.ds(pl.multiple_of((ids[1] // 2) * pair_rows, pair_rows), pair_rows), :]
    spill[...] = (own * spread).astype(BF16)
    payload[slots : slots + META, :] = jnp.zeros((META, edge), F32)
    slot_ids = lax.broadcasted_iota(jnp.int32, (1, slots), 1)
    payload[slots : slots + 1, 0:slots] = jnp.where(slot_ids < count[0], rows[...], -1).astype(F32)
    payload[slots + 1 : slots + 2, :] = jnp.sum(x * inv, axis=0, keepdims=True)


def first(layers, ids, cols_s, count, rows, values, gathered, payload, spill, xcur, inv_o, kinv_o,
          scaled, picked):
    slots, edge, _ = values.shape
    row_devices = gathered.shape[0]
    at = slots + META
    blocks = (gathered.shape[1] - at) // 2
    col_blk = row_devices * blocks
    degree = None
    block_ids = lax.broadcasted_iota(jnp.int32, (col_blk, slots), 0).astype(F32)
    for r in range(row_devices):
        onehot = (block_ids == gathered[r, slots : slots + 1, 0:slots]).astype(BF16)
        part = place(onehot, gathered[r, 0:slots, :])
        degree = part if degree is None else degree + part
    x = jnp.concatenate([gathered[r, at : at + blocks, :] for r in range(row_devices)], axis=0)
    keep = jnp.concatenate(
        [gathered[r, at + blocks : at + 2 * blocks, :] for r in range(row_devices)], axis=0
    )
    inv = 1.0 / (keep * degree + 1.0)
    kinv = keep * inv
    inv_o[...] = inv
    kinv_o[...] = kinv
    xcur[...] = x
    send_out(ids, layers, 2 * blocks, x, inv, kinv, rows, count, payload, spill, scaled, xcur)
    products(values, cols_s, scaled, picked, payload)


def joined(gathered):
    pairs = [gathered[2 * k] + gathered[2 * k + 1] for k in range(gathered.shape[0] // 2)]
    return pairs[0] if len(pairs) == 1 else jnp.concatenate(pairs, axis=0)


def middle(layers, ids, cols_s, count, rows, values, gathered, inv_i, kinv_i, xold, payload, spill,
           xcur, scaled, picked):
    slots, edge, _ = values.shape
    x = joined(gathered)
    xcur[...] = x
    send_out(ids, layers, gathered.shape[1], x, inv_i[...], kinv_i[...], rows, count, payload,
             spill, scaled, xcur)
    payload[slots + 2 : slots + 3, :] = jnp.sum(jnp.abs(x - xold[...]), axis=0, keepdims=True)
    products(values, cols_s, scaled, picked, payload)


def partial(node_total, ids, spill, *rest):
    pays, (part, change) = rest[:-2], rest[-2:]
    edge = part.shape[1]
    slots = pays[0].shape[0] - META
    blocks = part.shape[0] // 2
    first_block = (ids[2] * blocks).astype(F32)
    block_ids = lax.broadcasted_iota(jnp.int32, (blocks, slots), 0).astype(F32) + first_block
    walk, sums = None, None
    for pay in pays:
        onehot = (block_ids == pay[slots : slots + 1, 0:slots]).astype(BF16)
        got = place(onehot, pay[0:slots, :])
        meta = pay[slots : slots + META, :]
        walk = got if walk is None else walk + got
        sums = meta if sums is None else sums + meta
    mass = jnp.sum(sums[1:2, :], axis=1, keepdims=True)
    change[...] = sums
    base = damping * ((1.0 - coupling) * (walk + mass / node_total)) + (1.0 - damping)
    part[...] = damping * spill[...].astype(F32)
    mine = pl.ds(pl.multiple_of((ids[1] % 2) * blocks, blocks), blocks)
    part[mine, :] = part[mine, :] + base


def closing(ids, gathered, xold, ranks, change, xnew):
    edge = gathered.shape[2]
    wide = edge // 128
    x = joined(gathered)
    xnew[...] = x
    blocks = gathered.shape[1] // 2
    own = xnew[pl.ds(pl.multiple_of(ids[1] * blocks, blocks), blocks), :]
    for w in range(wide):
        ranks[pl.ds(w, blocks, wide), :] = own[:, w * 128 : (w + 1) * 128]
    change[...] = jnp.broadcast_to(
        jnp.sum(jnp.abs(x - xold[...]), axis=0, keepdims=True), change.shape
    )


def totals(*refs):
    early, late, out = refs[: ITERS - 1], refs[ITERS - 1 : -1], refs[-1]
    rows = [ref[2:3, :] for ref in early] + [sum(ref[0:1, :] for ref in late)]
    out[...] = jnp.concatenate([jnp.sum(row, axis=1, keepdims=True) for row in rows], axis=0)


def to_others(x, axis):
    size = lax.axis_size(axis)
    got = []
    for step in range(size - 1, 0, -1):
        if size & (size - 1):
            pairs = [(i, (i + step) % size) for i in range(size)]
        else:
            pairs = [(i, i ^ step) for i in range(size)]
        got.append(lax.ppermute(x, axis, pairs))
    return got


def to_layers(spill):
    layers, rows = lax.axis_size("layer"), lax.axis_size("row")
    pairs = []
    for layer in range(layers):
        for row in range(rows):
            other = layer + 1 if row % 2 == 0 else layer - 1
            if 0 <= other < layers:
                pairs.append((layer * rows + row, other * rows + row))
    return lax.ppermute(spill, ("layer", "row"), pairs)


def local(block_values, block_rows, block_cols, block_count, dangling, start_ranks):
    slots, edge = block_values.shape[3], block_values.shape[-1]
    span = start_ranks.shape[-1]
    row_devices = lax.axis_size("row")
    layers = lax.axis_size("layer")
    node_total = row_devices * lax.axis_size("col") * span
    blocks = span // edge
    col_blk = row_devices * blocks
    values = block_values.reshape(slots, edge, edge)
    rows = block_rows.reshape(1, slots)
    cols = block_cols.reshape(1, slots)
    cols_s = block_cols.reshape(slots)
    count = block_count.reshape(1)
    ids = jnp.stack([lax.axis_index("layer"), lax.axis_index("row"), lax.axis_index("col")])
    ids = ids.astype(jnp.int32)

    def shape(n, dtype=F32):
        return jax.ShapeDtypeStruct((n, edge), dtype)

    opened = call(
        opening, "opening", shape(slots + META + 2 * blocks), (VMEM, VMEM, SMEM, VMEM, VMEM)
    )(values, cols, count, start_ranks.reshape(-1, 128), dangling.reshape(-1, 128))
    gathered = lax.all_gather(opened, "row", axis=0)
    scratch = [pltpu.VMEM((col_blk, edge), F32), pltpu.VMEM((slots, edge), F32)]
    sent = (shape(slots + META), shape(2 * blocks, BF16), shape(col_blk))
    head = (SMEM, SMEM, SMEM, VMEM, VMEM, VMEM)
    payload, spill, x, inv, kinv = call(
        functools.partial(first, layers), "first", sent + (shape(col_blk), shape(col_blk)), head,
        scratch,
    )(ids, cols_s, count, rows, values, gathered)
    changes = []
    for t in range(ITERS):
        if t:
            payload, spill, x = call(
                functools.partial(middle, layers), "middle", sent, head + (VMEM, VMEM, VMEM),
                scratch,
            )(ids, cols_s, count, rows, values, gathered, inv, kinv, x)
        arriving = to_layers(spill)
        others = to_others(payload, "col")
        part, change = call(
            functools.partial(partial, node_total), "partial",
            (shape(2 * blocks), shape(META)),
            (SMEM, VMEM) + (VMEM,) * (1 + len(others)),
        )(ids, arriving, payload, *others)
        changes.append(change)
        gathered = lax.all_gather(part, "row", axis=0)
    ranks, last = call(
        closing, "closing", (jax.ShapeDtypeStruct((span // 128, 128), F32), shape(META)),
        (SMEM, VMEM, VMEM), [pltpu.VMEM((col_blk, edge), F32)],
    )(ids, gathered, x)
    lates = [last] + to_others(last, "col")
    residuals = call(
        totals, "totals", jax.ShapeDtypeStruct((ITERS, 1), F32),
        (VMEM,) * (ITERS - 1 + len(lates)),
    )(*changes[1:], *lates)
    return ranks.reshape(start_ranks.shape), residuals


def solution(mesh):
    placed = (
        P("layer", "row", "col", None, None, None),
        P("layer", "row", "col", None),
        P("layer", "row", "col", None),
        P("layer", "row", "col"),
        P("layer", "row", "col", None),
        P("layer", "row", "col", None),
    )
    return jax.shard_map(
        local,
        mesh=mesh,
        in_specs=placed,
        out_specs=(P("layer", "row", "col", None), P(None, "layer")),
        check_vma=False,
    )
```

```python
import functools
import jax
import jax.numpy as jnp
from jax import lax
from jax.experimental import pallas as pl
from jax.experimental.pallas import tpu as pltpu
from jax.sharding import PartitionSpec as P

ITERS = 3
damping = 0.85
coupling = 0.3

F32 = jnp.float32
BF16 = jnp.bfloat16
VMEM = pl.BlockSpec(memory_space=pltpu.VMEM)
SMEM = pl.BlockSpec(memory_space=pltpu.SMEM)
HBM = pl.BlockSpec(memory_space=pltpu.HBM)
META = 8
CHUNKS = 8


def call(body, name, outs, specs, scratch=(), aliases={}):
    return pl.pallas_call(
        body,
        name=name,
        out_shape=outs,
        in_specs=specs,
        out_specs=(VMEM,) * len(outs) if isinstance(outs, tuple) else VMEM,
        scratch_shapes=scratch,
        input_output_aliases=aliases,
        compiler_params=pltpu.CompilerParams(vmem_limit_bytes=24 * 1024 * 1024),
    )


def two_terms(x):
    hi = x.astype(BF16)
    return hi, (x - hi.astype(F32)).astype(BF16)


def place(onehot, rows):
    hi, lo = two_terms(rows)
    return jnp.dot(onehot, hi, preferred_element_type=F32) + jnp.dot(
        onehot, lo, preferred_element_type=F32
    )


def to_blocks(ref, edge):
    wide = edge // 128
    count = ref.shape[0] // wide
    return jnp.concatenate([ref[pl.ds(w, count, wide), :] for w in range(wide)], axis=1)


def opening(_, values_h, cols_h, count, x_h, dangling_h, out, values, cols, x, dangling, sems):
    slots, edge, _ = values.shape
    blocks = x.shape[0] * 128 // edge
    small = [
        pltpu.make_async_copy(source, target, sems.at[k])
        for k, (source, target) in enumerate(((cols_h, cols), (x_h, x), (dangling_h, dangling)))
    ]
    step = slots // CHUNKS
    large = [
        pltpu.make_async_copy(
            values_h.at[pl.ds(k * step, step)], values.at[pl.ds(k * step, step)], sems.at[3 + k]
        )
        for k in range(CHUNKS)
    ]
    for copy in small + large:
        copy.start()
    for copy in small:
        copy.wait()
    out[0, slots : slots + META, :] = jnp.zeros((META, edge), F32)
    slot_ids = lax.broadcasted_iota(jnp.int32, (1, slots), 1)
    out[0, slots : slots + 1, 0:slots] = jnp.where(slot_ids < count[0], cols[...], -1).astype(F32)
    at = slots + META
    out[0, at : at + blocks, :] = to_blocks(x, edge)
    out[0, at + blocks : at + 2 * blocks, :] = 1.0 - to_blocks(dangling, edge).astype(F32)
    ones = jnp.ones((16, edge), BF16)
    for k in range(CHUNKS):
        large[k].wait()
        for s in range(k * step, (k + 1) * step):
            got = jnp.dot(ones, values[s], preferred_element_type=F32)
            out[0, s : s + 1, :] = got[0:1, :]


def products(values, cols_s, scaled, picked, payload):
    slots = values.shape[0]
    for s in range(slots):
        picked[s : s + 1, :] = scaled[pl.ds(cols_s[s], 1), :]
    group = 16
    for g in range(slots // group):
        lhs = picked[g * group : (g + 1) * group, :].astype(BF16)
        for k in range(group):
            s = g * group + k
            got = lax.dot_general(
                lhs, values[s], (((1,), (1,)), ((), ())), preferred_element_type=F32
            )
            payload[s : s + 1, :] = got[k : k + 1, :]


def send_out(ids, layers, pair_rows, x, inv, kinv, rows, count, payload, spill, scaled, xcur):
    slots = rows.shape[1]
    edge = x.shape[1]
    scaled[...] = (x * kinv).astype(BF16).astype(F32)
    layer = ids[0]
    spread = jnp.where((layer == 0) | (layer == layers - 1), 1.0, 0.5).astype(F32) * coupling
    if x.shape[0] == pair_rows:
        own = x
    else:
        own = xcur[pl.ds(pl.multiple_of((ids[1] // 2) * pair_rows, pair_rows), pair_rows), :]
    spill[...] = (own * spread).astype(BF16)
    payload[slots : slots + META, :] = jnp.zeros((META, edge), F32)
    slot_ids = lax.broadcasted_iota(jnp.int32, (1, slots), 1)
    payload[slots : slots + 1, 0:slots] = jnp.where(slot_ids < count[0], rows[...], -1).astype(F32)
    payload[slots + 1 : slots + 2, :] = jnp.sum(x * inv, axis=0, keepdims=True)


def first(layers, ids, cols_s, count, rows, values, *rest):
    shared, (payload, spill, xcur, inv_o, kinv_o, scaled, picked) = rest[:-7], rest[-7:]
    slots, edge, _ = values.shape
    at = slots + META
    blocks = (shared[0].shape[1] - at) // 2
    if len(shared) == 1:
        parts = [(shared[0].at[r], r) for r in range(shared[0].shape[0])]
    else:
        parts = [(shared[0].at[0], ids[1]), (shared[1].at[0], 1 - ids[1])]
    degree = None
    block_ids = lax.broadcasted_iota(jnp.int32, (xcur.shape[0], slots), 0).astype(F32)
    for ref, row in parts:
        onehot = (block_ids == ref[slots : slots + 1, 0:slots]).astype(BF16)
        part = place(onehot, ref[0:slots, :])
        degree = part if degree is None else degree + part
        mine = pl.ds(row * blocks if isinstance(row, int) else pl.multiple_of(row * blocks, blocks), blocks)
        xcur[mine, :] = ref[at : at + blocks, :]
        kinv_o[mine, :] = ref[at + blocks : at + 2 * blocks, :]
    x, keep = xcur[...], kinv_o[...]
    inv = 1.0 / (keep * degree + 1.0)
    kinv = keep * inv
    inv_o[...] = inv
    kinv_o[...] = kinv
    send_out(ids, layers, 2 * blocks, x, inv, kinv, rows, count, payload, spill, scaled, xcur)
    products(values, cols_s, scaled, picked, payload)


def joined(parts):
    parts = [ref[k] for ref in parts for k in range(ref.shape[0])]
    pairs = [parts[2 * k] + parts[2 * k + 1] for k in range(len(parts) // 2)]
    return pairs[0] if len(pairs) == 1 else jnp.concatenate(pairs, axis=0)


def middle(layers, ids, cols_s, count, rows, values, inv_i, kinv_i, xold, *rest):
    shared, (payload, spill, xcur, scaled, picked) = rest[:-5], rest[-5:]
    slots, edge, _ = values.shape
    x = joined(shared)
    xcur[...] = x
    send_out(ids, layers, shared[0].shape[1], x, inv_i[...], kinv_i[...], rows, count, payload,
             spill, scaled, xcur)
    payload[slots + 2 : slots + 3, :] = jnp.sum(jnp.abs(x - xold[...]), axis=0, keepdims=True)
    products(values, cols_s, scaled, picked, payload)


def partial(layers, node_total, early, ids, spill, *rest):
    pays, outs = (rest[:-1], rest[-1:]) if early else (rest[:-2], rest[-2:])
    part = outs[0].at[0]
    edge = part.shape[1]
    slots = pays[0].shape[0] - META
    blocks = part.shape[0] // 2
    first_block = (ids[2] * blocks).astype(F32)
    block_ids = lax.broadcasted_iota(jnp.int32, (blocks, slots), 0).astype(F32) + first_block
    walk, sums = None, None
    for pay in pays:
        onehot = (block_ids == pay[slots : slots + 1, 0:slots]).astype(BF16)
        got = place(onehot, pay[0:slots, :])
        meta = pay[slots : slots + META, :]
        walk = got if walk is None else walk + got
        sums = meta if sums is None else sums + meta
    mass = jnp.sum(sums[1:2, :], axis=1, keepdims=True)
    if not early:
        outs[1][...] = sums
    base = damping * ((1.0 - coupling) * (walk + mass / node_total)) + (1.0 - damping)
    end = jnp.where(ids[1] % 2 == 0, 0, layers - 1)
    part[...] = jnp.where(ids[0] == end, 0.0, damping * spill[...].astype(F32))
    mine = pl.ds(pl.multiple_of((ids[1] % 2) * blocks, blocks), blocks)
    part[mine, :] = part[mine, :] + base


def closing(ids, xold, *rest):
    shared, (ranks, change, xnew) = rest[:-3], rest[-3:]
    edge = xold.shape[1]
    wide = edge // 128
    x = joined(shared)
    xnew[...] = x
    blocks = shared[0].shape[1] // 2
    own = xnew[pl.ds(pl.multiple_of(ids[1] * blocks, blocks), blocks), :]
    for w in range(wide):
        ranks[pl.ds(w, blocks, wide), :] = own[:, w * 128 : (w + 1) * 128]
    change[...] = jnp.broadcast_to(
        jnp.sum(jnp.abs(x - xold[...]), axis=0, keepdims=True), change.shape
    )


def totals(*refs):
    early, late, out = refs[: ITERS - 1], refs[ITERS - 1 : -1], refs[-1]
    rows = [ref[2:3, :] for ref in early] + [sum(ref[0:1, :] for ref in late)]
    out[...] = jnp.concatenate([jnp.sum(row, axis=1, keepdims=True) for row in rows], axis=0)


def to_others(x, axis):
    size = lax.axis_size(axis)
    got = []
    for step in range(1, size):
        if size & (size - 1):
            pairs = [(i, (i + step) % size) for i in range(size)]
        else:
            pairs = [(i, i ^ step) for i in range(size)]
        got.append(lax.ppermute(x, axis, pairs))
    return got


def to_rows(x):
    rows = lax.axis_size("row")
    if rows == 2:
        return x, lax.ppermute(x, "row", [(0, 1), (1, 0)])
    return (lax.all_gather(x, "row", axis=0, tiled=True),)


def to_layers(spill):
    layers, rows = lax.axis_size("layer"), lax.axis_size("row")
    pairs = []
    for layer in range(layers):
        for row in range(rows):
            other = layer + 1 if row % 2 == 0 else layer - 1
            if 0 <= other < layers:
                pairs.append((layer * rows + row, other * rows + row))
            else:
                pairs.append((layer * rows + row, layer * rows + (row ^ 1)))
    return lax.ppermute(spill, ("layer", "row"), pairs)


def local(block_values, block_rows, block_cols, block_count, dangling, start_ranks):
    slots, edge = block_values.shape[3], block_values.shape[-1]
    span = start_ranks.shape[-1]
    row_devices = lax.axis_size("row")
    layers = lax.axis_size("layer")
    node_total = row_devices * lax.axis_size("col") * span
    blocks = span // edge
    col_blk = row_devices * blocks
    values = block_values.reshape(slots, edge, edge)
    rows = block_rows.reshape(1, slots)
    cols = block_cols.reshape(1, slots)
    cols_s = block_cols.reshape(slots)
    count = block_count.reshape(1)
    ids = jnp.stack([lax.axis_index("layer"), lax.axis_index("row"), lax.axis_index("col")])
    ids = ids.astype(jnp.int32)

    def shape(n, dtype=F32):
        return jax.ShapeDtypeStruct((n, edge), dtype)

    def lead(n):
        return jax.ShapeDtypeStruct((1, n, edge), F32)

    flat = (span // 128, 128)
    def far(x):
        return pltpu.with_memory_space_constraint(x, pltpu.HBM)

    opened, values = call(
        opening, "opening",
        (lead(slots + META + 2 * blocks), pltpu.VMEM(values.shape, BF16)),
        (SMEM, HBM, HBM, SMEM, HBM, HBM),
        [pltpu.VMEM((1, slots), jnp.int32), pltpu.VMEM(flat, F32), pltpu.VMEM(flat, jnp.int32),
         pltpu.SemaphoreType.DMA((3 + CHUNKS,))],
    )(ids, far(values), far(cols), count, far(start_ranks.reshape(flat)), far(dangling.reshape(flat)))
    shared = to_rows(opened)
    scratch = [pltpu.VMEM((col_blk, edge), F32), pltpu.VMEM((slots, edge), F32)]
    sent = (shape(slots + META), shape(2 * blocks, BF16), shape(col_blk))
    head = (SMEM, SMEM, SMEM, VMEM, VMEM)
    payload, spill, x, inv, kinv = call(
        functools.partial(first, layers), "first", sent + (shape(col_blk), shape(col_blk)),
        head + (VMEM,) * len(shared), scratch,
    )(ids, cols_s, count, rows, values, *shared)
    changes = []
    for t in range(ITERS):
        if t:
            payload, spill, x = call(
                functools.partial(middle, layers), "middle", sent,
                head + (VMEM,) * (3 + len(shared)), scratch,
            )(ids, cols_s, count, rows, values, inv, kinv, x, *shared)
        arriving = to_layers(spill)
        others = to_others(payload, "col")
        part, *change = call(
            functools.partial(partial, layers, node_total, t == 0), "partial",
            (lead(2 * blocks), shape(META))[: 1 + (t > 0)],
            (SMEM, VMEM) + (VMEM,) * (1 + len(others)),
        )(ids, arriving, payload, *others)
        changes += change
        shared = to_rows(part)
    ranks, last = call(
        closing, "closing", (jax.ShapeDtypeStruct(flat, F32), shape(META)),
        (SMEM, VMEM) + (VMEM,) * len(shared), [pltpu.VMEM((col_blk, edge), F32)],
    )(ids, x, *shared)
    lates = [last] + to_others(last, "col")
    residuals = call(
        totals, "totals", jax.ShapeDtypeStruct((ITERS, 1), F32),
        (VMEM,) * (ITERS - 1 + len(lates)),
    )(*changes, *lates)
    return ranks.reshape(start_ranks.shape), residuals


def solution(mesh):
    placed = (
        P("layer", "row", "col", None, None, None),
        P("layer", "row", "col", None),
        P("layer", "row", "col", None),
        P("layer", "row", "col"),
        P("layer", "row", "col", None),
        P("layer", "row", "col", None),
    )
    return jax.shard_map(
        local,
        mesh=mesh,
        in_specs=placed,
        out_specs=(P("layer", "row", "col", None), P(None, "layer")),
        check_vma=False,
    )
```

```python
import functools
import jax
import jax.numpy as jnp
from jax import lax
from jax.experimental import pallas as pl
from jax.experimental.pallas import tpu as pltpu
from jax.sharding import PartitionSpec as P

ITERS = 3
damping = 0.85
coupling = 0.3

F32 = jnp.float32
BF16 = jnp.bfloat16
VMEM = pl.BlockSpec(memory_space=pltpu.VMEM)
SMEM = pl.BlockSpec(memory_space=pltpu.SMEM)
HBM = pl.BlockSpec(memory_space=pltpu.HBM)
META = 8
CHUNKS = 8


def call(body, outs, specs, scratch=(), aliases={}):
    return pl.pallas_call(
        body,
        out_shape=outs,
        in_specs=specs,
        out_specs=(VMEM,) * len(outs) if isinstance(outs, tuple) else VMEM,
        scratch_shapes=scratch,
        input_output_aliases=aliases,
        compiler_params=pltpu.CompilerParams(vmem_limit_bytes=24 * 1024 * 1024),
    )


def two_terms(x):
    hi = x.astype(BF16)
    return hi, (x - hi.astype(F32)).astype(BF16)


def place(onehot, rows):
    hi, lo = two_terms(rows)
    return jnp.dot(onehot, hi, preferred_element_type=F32) + jnp.dot(
        onehot, lo, preferred_element_type=F32
    )


def to_blocks(ref, edge):
    wide = edge // 128
    count = ref.shape[0] // wide
    return jnp.concatenate([ref[pl.ds(w, count, wide), :] for w in range(wide)], axis=1)


def opening(_, values_h, cols_h, count, x_h, dangling_h, out, values, cols, x, dangling, sems):
    slots, edge, _ = values.shape
    blocks = x.shape[0] * 128 // edge
    small = [
        pltpu.make_async_copy(source, target, sems.at[k])
        for k, (source, target) in enumerate(((cols_h, cols), (x_h, x), (dangling_h, dangling)))
    ]
    step = slots // CHUNKS
    large = [
        pltpu.make_async_copy(
            values_h.at[pl.ds(k * step, step)], values.at[pl.ds(k * step, step)], sems.at[3 + k]
        )
        for k in range(CHUNKS)
    ]
    for copy in small + large:
        copy.start()
    for copy in small:
        copy.wait()
    out[0, slots : slots + META, :] = jnp.zeros((META, edge), F32)
    slot_ids = lax.broadcasted_iota(jnp.int32, (1, slots), 1)
    out[0, slots : slots + 1, 0:slots] = jnp.where(slot_ids < count[0], cols[...], -1).astype(F32)
    at = slots + META
    out[0, at : at + blocks, :] = to_blocks(x, edge)
    out[0, at + blocks : at + 2 * blocks, :] = 1.0 - to_blocks(dangling, edge).astype(F32)
    ones = jnp.ones((16, edge), BF16)
    for k in range(CHUNKS):
        large[k].wait()
        for s in range(k * step, (k + 1) * step):
            got = jnp.dot(ones, values[s], preferred_element_type=F32)
            out[0, s : s + 1, :] = got[0:1, :]


def products(values, cols_s, scaled, picked, payload):
    slots = values.shape[0]
    for s in range(slots):
        picked[s : s + 1, :] = scaled[pl.ds(cols_s[s], 1), :]
    group = 16
    for g in range(slots // group):
        lhs = picked[g * group : (g + 1) * group, :].astype(BF16)
        for k in range(group):
            s = g * group + k
            got = lax.dot_general(
                lhs, values[s], (((1,), (1,)), ((), ())), preferred_element_type=F32
            )
            payload[s : s + 1, :] = got[k : k + 1, :]


def send_out(ids, layers, pair_rows, x, inv, kinv, rows, count, payload, spill, scaled, xcur):
    slots = rows.shape[1]
    edge = x.shape[1]
    scaled[...] = (x * kinv).astype(BF16).astype(F32)
    layer = ids[0]
    spread = jnp.where((layer == 0) | (layer == layers - 1), 1.0, 0.5).astype(F32) * coupling
    if x.shape[0] == pair_rows:
        own = x
    else:
        own = xcur[pl.ds(pl.multiple_of((ids[1] // 2) * pair_rows, pair_rows), pair_rows), :]
    spill[...] = (own * spread).astype(BF16)
    payload[slots : slots + META, :] = jnp.zeros((META, edge), F32)
    slot_ids = lax.broadcasted_iota(jnp.int32, (1, slots), 1)
    payload[slots : slots + 1, 0:slots] = jnp.where(slot_ids < count[0], rows[...], -1).astype(F32)
    payload[slots + 1 : slots + 2, :] = jnp.sum(x * inv, axis=0, keepdims=True)


def first(layers, ids, cols_s, count, rows, values, *rest):
    shared, (payload, spill, xcur, inv_o, kinv_o, scaled, picked) = rest[:-7], rest[-7:]
    slots, _, _ = values.shape
    at = slots + META
    blocks = (shared[0].shape[1] - at) // 2
    if len(shared) == 1:
        parts = [(shared[0].at[r], r) for r in range(shared[0].shape[0])]
    else:
        parts = [(shared[0].at[0], ids[1]), (shared[1].at[0], 1 - ids[1])]
    degree = None
    block_ids = lax.broadcasted_iota(jnp.int32, (xcur.shape[0], slots), 0).astype(F32)
    for ref, row in parts:
        onehot = (block_ids == ref[slots : slots + 1, 0:slots]).astype(BF16)
        part = place(onehot, ref[0:slots, :])
        degree = part if degree is None else degree + part
        mine = pl.ds(row * blocks if isinstance(row, int) else pl.multiple_of(row * blocks, blocks), blocks)
        xcur[mine, :] = ref[at : at + blocks, :]
        kinv_o[mine, :] = ref[at + blocks : at + 2 * blocks, :]
    x, keep = xcur[...], kinv_o[...]
    inv = 1.0 / (keep * degree + 1.0)
    kinv = keep * inv
    inv_o[...] = inv
    kinv_o[...] = kinv
    send_out(ids, layers, 2 * blocks, x, inv, kinv, rows, count, payload, spill, scaled, xcur)
    products(values, cols_s, scaled, picked, payload)


def joined(parts):
    parts = [ref[k] for ref in parts for k in range(ref.shape[0])]
    pairs = [parts[2 * k] + parts[2 * k + 1] for k in range(len(parts) // 2)]
    return pairs[0] if len(pairs) == 1 else jnp.concatenate(pairs, axis=0)


def middle(layers, ids, cols_s, count, rows, values, inv_i, kinv_i, xold, *rest):
    shared, (payload, spill, xcur, scaled, picked) = rest[:-5], rest[-5:]
    slots, _, _ = values.shape
    x = joined(shared)
    xcur[...] = x
    send_out(ids, layers, shared[0].shape[1], x, inv_i[...], kinv_i[...], rows, count, payload,
             spill, scaled, xcur)
    payload[slots + 2 : slots + 3, :] = jnp.sum(jnp.abs(x - xold[...]), axis=0, keepdims=True)
    products(values, cols_s, scaled, picked, payload)


def partial(layers, node_total, early, ids, spill, *rest):
    pays, outs = (rest[:-1], rest[-1:]) if early else (rest[:-2], rest[-2:])
    part = outs[0].at[0]
    slots = pays[0].shape[0] - META
    blocks = part.shape[0] // 2
    first_block = (ids[2] * blocks).astype(F32)
    block_ids = lax.broadcasted_iota(jnp.int32, (blocks, slots), 0).astype(F32) + first_block
    walks, sums = [], None
    for pay in pays:
        onehot = (block_ids == pay[slots : slots + 1, 0:slots]).astype(BF16)
        walks.append(place(onehot, pay[0:slots, :]))
        meta = pay[slots : slots + META, :]
        sums = meta if sums is None else sums + meta
    mass = jnp.sum(sums[1:2, :], axis=1, keepdims=True)
    if not early:
        outs[1][...] = sums
    end = jnp.where(ids[1] % 2 == 0, layers - 1, 0)
    part[...] = jnp.where(ids[0] == end, 0.0, damping * spill[...].astype(F32))
    walk = damping * (1.0 - coupling)
    own = pl.ds(pl.multiple_of((ids[1] % 2) * blocks, blocks), blocks)
    peer = pl.ds(pl.multiple_of((1 - ids[1] % 2) * blocks, blocks), blocks)
    part[own, :] = part[own, :] + (walk * (walks[0] + mass / node_total) + (1.0 - damping))
    part[peer, :] = part[peer, :] + walk * sum(walks[1:])


def closing(ids, xold, *rest):
    shared, (ranks, change, xnew) = rest[:-3], rest[-3:]
    edge = xold.shape[1]
    wide = edge // 128
    x = joined(shared)
    xnew[...] = x
    blocks = shared[0].shape[1] // 2
    own = xnew[pl.ds(pl.multiple_of(ids[1] * blocks, blocks), blocks), :]
    for w in range(wide):
        ranks[pl.ds(w, blocks, wide), :] = own[:, w * 128 : (w + 1) * 128]
    change[...] = jnp.broadcast_to(
        jnp.sum(jnp.abs(x - xold[...]), axis=0, keepdims=True), change.shape
    )


def totals(*refs):
    early, late, out = refs[: ITERS - 1], refs[ITERS - 1 : -1], refs[-1]
    rows = [ref[2:3, :] for ref in early] + [sum(ref[0:1, :] for ref in late)]
    out[...] = jnp.concatenate([jnp.sum(row, axis=1, keepdims=True) for row in rows], axis=0)


def to_others(x):
    rows, cols = lax.axis_size("row"), lax.axis_size("col")
    got = []
    for step in range(1, cols):
        pairs = []
        for row in range(rows):
            for col in range(cols):
                other = (col + step) % cols if cols & (cols - 1) else col ^ step
                pairs.append((row * cols + col, (row ^ 1) * cols + other))
        got.append(lax.ppermute(x, ("row", "col"), pairs))
    return got


def to_rows(x):
    rows = lax.axis_size("row")
    if rows == 2:
        return x, lax.ppermute(x, "row", [(0, 1), (1, 0)])
    return (lax.all_gather(x, "row", axis=0, tiled=True),)


def to_layers(spill):
    layers, rows = lax.axis_size("layer"), lax.axis_size("row")
    pairs = []
    for layer in range(layers):
        for row in range(rows):
            other = (layer + 1) % layers if row % 2 == 0 else (layer - 1) % layers
            pairs.append((layer * rows + row, other * rows + (row ^ 1)))
    return lax.ppermute(spill, ("layer", "row"), pairs)


def local(block_values, block_rows, block_cols, block_count, dangling, start_ranks):
    slots, edge = block_values.shape[3], block_values.shape[-1]
    span = start_ranks.shape[-1]
    row_devices = lax.axis_size("row")
    layers = lax.axis_size("layer")
    node_total = row_devices * lax.axis_size("col") * span
    blocks = span // edge
    col_blk = row_devices * blocks
    values = block_values.reshape(slots, edge, edge)
    rows = block_rows.reshape(1, slots)
    cols = block_cols.reshape(1, slots)
    cols_s = block_cols.reshape(slots)
    count = block_count.reshape(1)
    ids = jnp.stack([lax.axis_index("layer"), lax.axis_index("row"), lax.axis_index("col")])
    ids = ids.astype(jnp.int32)

    def shape(n, dtype=F32):
        return jax.ShapeDtypeStruct((n, edge), dtype)

    def lead(n):
        return jax.ShapeDtypeStruct((1, n, edge), F32)

    flat = (span // 128, 128)

    def far(x):
        return pltpu.with_memory_space_constraint(x, pltpu.HBM)

    opened, values = call(
        opening,
        (lead(slots + META + 2 * blocks), pltpu.VMEM(values.shape, BF16)),
        (SMEM, HBM, HBM, SMEM, HBM, HBM),
        [pltpu.VMEM((1, slots), jnp.int32), pltpu.VMEM(flat, F32), pltpu.VMEM(flat, jnp.int32),
         pltpu.SemaphoreType.DMA((3 + CHUNKS,))],
    )(ids, far(values), far(cols), count, far(start_ranks.reshape(flat)), far(dangling.reshape(flat)))
    shared = to_rows(opened)
    scratch = [pltpu.VMEM((col_blk, edge), F32), pltpu.VMEM((slots, edge), F32)]
    sent = (shape(slots + META), shape(2 * blocks, BF16), shape(col_blk))
    head = (SMEM, SMEM, SMEM, VMEM, VMEM)
    payload, spill, x, inv, kinv = call(
        functools.partial(first, layers), sent + (shape(col_blk), shape(col_blk)),
        head + (VMEM,) * len(shared), scratch,
    )(ids, cols_s, count, rows, values, *shared)
    changes = []
    for t in range(ITERS):
        if t:
            payload, spill, x = call(
                functools.partial(middle, layers), sent,
                head + (VMEM,) * (3 + len(shared)), scratch,
            )(ids, cols_s, count, rows, values, inv, kinv, x, *shared)
        arriving = to_layers(spill)
        others = to_others(payload)
        part, *change = call(
            functools.partial(partial, layers, node_total, t == 0),
            (lead(2 * blocks), shape(META))[: 1 + (t > 0)],
            (SMEM, VMEM) + (VMEM,) * (1 + len(others)),
        )(ids, arriving, payload, *others)
        changes += change
        shared = to_rows(part)
    ranks, last = call(
        closing, (jax.ShapeDtypeStruct(flat, F32), shape(META)),
        (SMEM, VMEM) + (VMEM,) * len(shared), [pltpu.VMEM((col_blk, edge), F32)],
    )(ids, x, *shared)
    lates = [last] + to_others(last)
    residuals = call(
        totals, jax.ShapeDtypeStruct((ITERS, 1), F32),
        (VMEM,) * (ITERS - 1 + len(lates)),
    )(*changes, *lates)
    return ranks.reshape(start_ranks.shape), residuals


def solution(mesh):
    placed = (
        P("layer", "row", "col", None, None, None),
        P("layer", "row", "col", None),
        P("layer", "row", "col", None),
        P("layer", "row", "col"),
        P("layer", "row", "col", None),
        P("layer", "row", "col", None),
    )
    return jax.shard_map(
        local,
        mesh=mesh,
        in_specs=placed,
        out_specs=(P("layer", "row", "col", None), P(None, "layer")),
        check_vma=False,
    )
```

```python
import functools
import jax
import jax.numpy as jnp
from jax import lax
from jax.experimental import pallas as pl
from jax.experimental.pallas import tpu as pltpu
from jax.sharding import PartitionSpec as P

ITERS = 3
damping = 0.85
coupling = 0.3

F32 = jnp.float32
BF16 = jnp.bfloat16
VMEM = pl.BlockSpec(memory_space=pltpu.VMEM)
HBM = pl.BlockSpec(memory_space=pltpu.HBM)
META = 8
CHUNKS = 4


def call(body, outs, specs, scratch=(), aliases={}):
    return pl.pallas_call(
        body,
        out_shape=outs,
        in_specs=specs,
        out_specs=(VMEM,) * len(outs) if isinstance(outs, tuple) else VMEM,
        scratch_shapes=scratch,
        input_output_aliases=aliases,
        compiler_params=pltpu.CompilerParams(vmem_limit_bytes=24 * 1024 * 1024),
    )


def two_terms(x):
    hi = x.astype(BF16)
    return hi, (x - hi.astype(F32)).astype(BF16)


def place(onehot, rows):
    hi, lo = two_terms(rows)
    return jnp.dot(onehot, hi, preferred_element_type=F32) + jnp.dot(
        onehot, lo, preferred_element_type=F32
    )


def to_blocks(ref, edge):
    wide = edge // 128
    count = ref.shape[0] // wide
    return jnp.concatenate([ref[pl.ds(w, count, wide), :] for w in range(wide)], axis=1)


def opening(values_h, cols_h, rows_h, count_h, x_h, dangling_h, packed, turned, pick, marks,
            values, cols, rows, count, x, dangling, sems):
    slots, edge, _ = values.shape
    blocks = x.shape[0] * 128 // edge
    step = slots // CHUNKS
    large = [
        pltpu.make_async_copy(
            values_h.at[pl.ds(k * step, step)], values.at[pl.ds(k * step, step)], sems.at[k]
        )
        for k in range(CHUNKS)
    ]
    pairs = ((cols_h, cols), (rows_h, rows), (count_h, count), (x_h, x), (dangling_h, dangling))
    small = [
        pltpu.make_async_copy(source, target, sems.at[CHUNKS + k])
        for k, (source, target) in enumerate(pairs)
    ]
    for copy in small + large:
        copy.start()
    for copy in small:
        copy.wait()
    live = lax.broadcasted_iota(jnp.int32, (1, slots), 1) < count[...]
    packed[0, slots : slots + META, :] = jnp.zeros((META, edge), F32)
    packed[0, slots : slots + 1, 0:slots] = jnp.where(live, cols[...], -1).astype(F32)
    marks[...] = jnp.zeros((META, edge), F32)
    marks[0:1, 0:slots] = jnp.where(live, rows[...], -1).astype(F32)
    source_ids = lax.broadcasted_iota(jnp.int32, (pick.shape[1], slots), 0)
    pick[...] = (source_ids == cols[...]).astype(F32).T.astype(BF16)
    at = slots + META
    packed[0, at : at + blocks, :] = to_blocks(x, edge)
    packed[0, at + blocks : at + 2 * blocks, :] = 1.0 - to_blocks(dangling, edge).astype(F32)
    ones = jnp.ones((16, edge), BF16)
    for k in range(CHUNKS):
        large[k].wait()
        for s in range(k * step, (k + 1) * step):
            block = values[s]
            turned[s] = block.T
            got = jnp.dot(ones, block, preferred_element_type=F32)
            packed[0, s : s + 1, :] = got[0:1, :]


def send_out(layers, pair_rows, x, inv, kinv, turned, pick, marks, payload, spill, xcur):
    slots = turned.shape[0]
    scaled = (x * kinv).astype(BF16)
    picked = jnp.dot(pick[...], scaled, preferred_element_type=F32).astype(BF16)
    group = 16
    for g in range(slots // group):
        lhs = picked[g * group : (g + 1) * group, :]
        for k in range(group):
            s = g * group + k
            got = jnp.dot(lhs, turned[s], preferred_element_type=F32)
            payload[s : s + 1, :] = got[k : k + 1, :]
    payload[slots : slots + META, :] = marks[...]
    payload[slots + 1 : slots + 2, :] = jnp.sum(x * inv, axis=0, keepdims=True)
    layer = lax.axis_index("layer")
    spread = jnp.where((layer == 0) | (layer == layers - 1), 1.0, 0.5).astype(F32) * coupling
    if x.shape[0] == pair_rows:
        own = x
    else:
        first_row = pl.multiple_of((lax.axis_index("row") // 2) * pair_rows, pair_rows)
        own = xcur[pl.ds(first_row, pair_rows), :]
    spill[...] = (own * spread).astype(BF16)


def first(layers, turned, pick, marks, *rest):
    shared, (payload, spill, xcur, inv_o, kinv_o) = rest[:-5], rest[-5:]
    slots = turned.shape[0]
    at = slots + META
    blocks = (shared[0].shape[1] - at) // 2
    if len(shared) == 1:
        parts = [(shared[0].at[r], r * blocks) for r in range(shared[0].shape[0])]
    else:
        row = lax.axis_index("row")
        starts = (row * blocks, (1 - row) * blocks)
        parts = [(ref.at[0], pl.multiple_of(at, blocks)) for ref, at in zip(shared, starts)]
    degree = None
    block_ids = lax.broadcasted_iota(jnp.int32, (xcur.shape[0], slots), 0).astype(F32)
    for ref, start in parts:
        onehot = (block_ids == ref[slots : slots + 1, 0:slots]).astype(BF16)
        part = place(onehot, ref[0:slots, :])
        degree = part if degree is None else degree + part
        mine = pl.ds(start, blocks)
        xcur[mine, :] = ref[at : at + blocks, :]
        kinv_o[mine, :] = ref[at + blocks : at + 2 * blocks, :]
    x, keep = xcur[...], kinv_o[...]
    inv = 1.0 / (keep * degree + 1.0)
    kinv = keep * inv
    inv_o[...] = inv
    kinv_o[...] = kinv
    send_out(layers, 2 * blocks, x, inv, kinv, turned, pick, marks, payload, spill, xcur)


def joined(parts):
    parts = [ref[k] for ref in parts for k in range(ref.shape[0])]
    pairs = [parts[2 * k] + parts[2 * k + 1] for k in range(len(parts) // 2)]
    return pairs[0] if len(pairs) == 1 else jnp.concatenate(pairs, axis=0)


def lane_change(x, xold):
    return jnp.sum(jnp.abs(x - xold[...]), axis=0, keepdims=True)


def middle(layers, turned, pick, marks, inv_i, kinv_i, xold, *rest):
    shared, (payload, spill, xcur) = rest[:-3], rest[-3:]
    slots = turned.shape[0]
    x = joined(shared)
    xcur[...] = x
    send_out(layers, shared[0].shape[1], x, inv_i[...], kinv_i[...], turned, pick, marks, payload,
             spill, xcur)
    payload[slots + 2 : slots + 3, :] = lane_change(x, xold)


def partial(layers, node_total, early, spill, *rest):
    pays, outs = (rest[:-1], rest[-1:]) if early else (rest[:-2], rest[-2:])
    part = outs[0]
    slots = pays[0].shape[0] - META
    blocks = part.shape[1] // 2
    odd = lax.axis_index("row") % 2
    first_block = (lax.axis_index("col") * blocks).astype(F32)
    block_ids = lax.broadcasted_iota(jnp.int32, (blocks, slots), 0).astype(F32) + first_block
    walks, sums = [], None
    for pay in pays:
        onehot = (block_ids == pay[slots : slots + 1, 0:slots]).astype(BF16)
        walks.append(place(onehot, pay[0:slots, :]))
        meta = pay[slots : slots + META, :]
        sums = meta if sums is None else sums + meta
    mass = jnp.sum(sums[1:2, :], axis=1, keepdims=True)
    if not early:
        outs[1][...] = sums
    end = jnp.where(odd == 0, layers - 1, 0)
    arrive = jnp.where(lax.axis_index("layer") == end, 0.0, damping * spill[...].astype(F32))
    walk = damping * (1.0 - coupling)
    own = walk * (walks[0] + mass / node_total) + (1.0 - damping)
    peer = walk * sum(walks[1:])
    part[0, 0:blocks, :] = arrive[0:blocks] + jnp.where(odd == 0, own, peer)
    part[0, blocks:, :] = arrive[blocks:] + jnp.where(odd == 0, peer, own)


def closing(xold, *rest):
    shared, (xnew, change) = rest[:-2], rest[-2:]
    x = joined(shared)
    xnew[...] = x
    change[...] = jnp.broadcast_to(lane_change(x, xold), change.shape)


def flatten(xnew, ranks):
    wide = xnew.shape[1] // 128
    blocks = ranks.shape[0] // wide
    start = pl.multiple_of(lax.axis_index("row") * blocks, blocks)
    own = xnew[pl.ds(start, blocks), :]
    for w in range(wide):
        ranks[pl.ds(w, blocks, wide), :] = own[:, w * 128 : (w + 1) * 128]


def totals(*refs):
    early, late, out = refs[: ITERS - 1], refs[ITERS - 1 : -1], refs[-1]
    rows = [ref[2:3, :] for ref in early] + [sum(ref[0:1, :] for ref in late)]
    for t, row in enumerate(rows):
        out[0:1, t : t + 1] = jnp.sum(row, axis=1, keepdims=True)


def to_others(x):
    rows, cols = lax.axis_size("row"), lax.axis_size("col")
    got = []
    for step in range(1, cols):
        pairs = []
        for row in range(rows):
            for col in range(cols):
                other = (col + step) % cols if cols & (cols - 1) else col ^ step
                pairs.append((row * cols + col, (row ^ 1) * cols + other))
        got.append(lax.ppermute(x, ("row", "col"), pairs))
    return got


def to_rows(x):
    rows = lax.axis_size("row")
    if rows == 2:
        return x, lax.ppermute(x, "row", [(0, 1), (1, 0)])
    return (lax.all_gather(x, "row", axis=0, tiled=True),)


def to_layers(spill):
    layers, rows = lax.axis_size("layer"), lax.axis_size("row")
    pairs = []
    for layer in range(layers):
        for row in range(rows):
            other = (layer + 1) % layers if row % 2 == 0 else (layer - 1) % layers
            pairs.append((layer * rows + row, other * rows + (row ^ 1)))
    return lax.ppermute(spill, ("layer", "row"), pairs)


def local(block_values, block_rows, block_cols, block_count, dangling, start_ranks):
    slots, edge = block_values.shape[3], block_values.shape[-1]
    span = start_ranks.shape[-1]
    row_devices = lax.axis_size("row")
    layers = lax.axis_size("layer")
    node_total = row_devices * lax.axis_size("col") * span
    blocks = span // edge
    col_blk = row_devices * blocks
    flat = (span // 128, 128)
    arguments = [
        block_values.reshape(slots, edge, edge), block_cols.reshape(1, slots),
        block_rows.reshape(1, slots), block_count.reshape(1, 1), start_ranks.reshape(flat),
        dangling.reshape(flat),
    ]
    arguments = [
        x if x.size == 1 else pltpu.with_memory_space_constraint(x, pltpu.HBM) for x in arguments
    ]

    def shape(n, dtype=F32):
        return jax.ShapeDtypeStruct((n, edge), dtype)

    def lead(n):
        return jax.ShapeDtypeStruct((1, n, edge), F32)

    packed, turned, pick, marks = call(
        opening,
        (lead(slots + META + 2 * blocks), pltpu.VMEM((slots, edge, edge), BF16),
         pltpu.VMEM((slots, col_blk), BF16), pltpu.VMEM((META, edge), F32)),
        (HBM, HBM, HBM, pl.BlockSpec(memory_space=pl.ANY), HBM, HBM),
        [pltpu.VMEM((slots, edge, edge), BF16), pltpu.VMEM((1, slots), jnp.int32),
         pltpu.VMEM((1, slots), jnp.int32), pltpu.VMEM((1, 1), jnp.int32), pltpu.VMEM(flat, F32),
         pltpu.VMEM(flat, jnp.int32), pltpu.SemaphoreType.DMA((5 + CHUNKS,))],
    )(*arguments)
    shared = to_rows(packed)
    sent = (shape(slots + META), shape(2 * blocks, BF16), shape(col_blk))
    payload, spill, x, inv, kinv = call(
        functools.partial(first, layers), sent + (shape(col_blk), shape(col_blk)),
        (VMEM,) * (3 + len(shared)),
    )(turned, pick, marks, *shared)
    changes = []
    for t in range(ITERS):
        if t:
            payload, spill, x = call(
                functools.partial(middle, layers), sent, (VMEM,) * (6 + len(shared)),
            )(turned, pick, marks, inv, kinv, x, *shared)
        arriving = to_layers(spill)
        others = to_others(payload)
        part, *change = call(
            functools.partial(partial, layers, node_total, t == 0),
            (lead(2 * blocks), shape(META))[: 1 + (t > 0)], (VMEM,) * (2 + len(others)),
        )(arriving, payload, *others)
        changes += change
        shared = to_rows(part)
    xnew, last = call(
        closing, (shape(col_blk), shape(META)), (VMEM,) * (1 + len(shared))
    )(x, *shared)
    lates = [last] + to_others(last)
    ranks = call(flatten, jax.ShapeDtypeStruct(flat, F32), (VMEM,))(xnew)
    residuals = call(
        totals, jax.ShapeDtypeStruct((1, ITERS), F32),
        (VMEM,) * (ITERS - 1 + len(lates)),
    )(*changes, *lates)
    return ranks.reshape(start_ranks.shape), residuals.reshape(ITERS, 1)


def solution(mesh):
    placed = (
        P("layer", "row", "col", None, None, None),
        P("layer", "row", "col", None),
        P("layer", "row", "col", None),
        P("layer", "row", "col"),
        P("layer", "row", "col", None),
        P("layer", "row", "col", None),
    )
    return jax.shard_map(
        local,
        mesh=mesh,
        in_specs=placed,
        out_specs=(P("layer", "row", "col", None), P(None, "layer")),
        check_vma=False,
    )
```

```python
import functools
import jax
import jax.numpy as jnp
from jax import lax
from jax.experimental import pallas as pl
from jax.experimental.pallas import tpu as pltpu
from jax.sharding import PartitionSpec as P

ITERS = 3
damping = 0.85
coupling = 0.3

F32 = jnp.float32
BF16 = jnp.bfloat16
VMEM = pl.BlockSpec(memory_space=pltpu.VMEM)
HBM = pl.BlockSpec(memory_space=pltpu.HBM)
META = 8
LANES = 128
CHUNKS = 4


def call(body, outs, specs, scratch=(), aliases={}):
    return pl.pallas_call(
        body,
        out_shape=outs,
        in_specs=specs,
        out_specs=(VMEM,) * len(outs) if isinstance(outs, tuple) else VMEM,
        scratch_shapes=scratch,
        input_output_aliases=aliases,
        compiler_params=pltpu.CompilerParams(vmem_limit_bytes=24 * 1024 * 1024),
    )


def two_terms(x):
    hi = x.astype(BF16)
    return hi, (x - hi.astype(F32)).astype(BF16)


def place(onehot, rows):
    hi, lo = two_terms(rows)
    return jnp.dot(onehot, hi, preferred_element_type=F32) + jnp.dot(
        onehot, lo, preferred_element_type=F32
    )


def to_blocks(ref, edge):
    wide = edge // 128
    count = ref.shape[0] // wide
    return jnp.concatenate([ref[pl.ds(w, count, wide), :] for w in range(wide)], axis=1)


def opening(values_h, cols_h, rows_h, count_h, x_h, dangling_h, packed, turned, pick, marks,
            values, cols, rows, count, x, dangling, sems):
    slots, edge, _ = values.shape
    blocks = x.shape[0] * 128 // edge
    step = slots // CHUNKS
    large = [
        pltpu.make_async_copy(
            values_h.at[pl.ds(k * step, step)], values.at[pl.ds(k * step, step)], sems.at[k]
        )
        for k in range(CHUNKS)
    ]
    pairs = ((cols_h, cols), (rows_h, rows), (count_h, count), (x_h, x), (dangling_h, dangling))
    small = [
        pltpu.make_async_copy(source, target, sems.at[CHUNKS + k])
        for k, (source, target) in enumerate(pairs)
    ]
    for copy in small + large:
        copy.start()
    for copy in small:
        copy.wait()
    live = lax.broadcasted_iota(jnp.int32, (1, slots), 1) < count[...]
    packed[0, slots : slots + META, :] = jnp.zeros((META, edge), F32)
    packed[0, slots : slots + 1, 0:slots] = jnp.where(live, cols[...], -1).astype(F32)
    marks[...] = jnp.zeros((META, LANES), F32)
    marks[0:1, 0:slots] = jnp.where(live, rows[...], -1).astype(F32)
    source_ids = lax.broadcasted_iota(jnp.int32, (pick.shape[1], slots), 0)
    pick[...] = (source_ids == cols[...]).astype(F32).T.astype(BF16)
    at = slots + META
    packed[0, at : at + blocks, :] = to_blocks(x, edge)
    packed[0, at + blocks : at + 2 * blocks, :] = 1.0 - to_blocks(dangling, edge).astype(F32)
    ones = jnp.ones((16, edge), BF16)
    for k in range(CHUNKS):
        large[k].wait()
        for s in range(k * step, (k + 1) * step):
            block = values[s]
            turned[s] = block.T
            got = jnp.dot(ones, block, preferred_element_type=F32)
            packed[0, s : s + 1, :] = got[0:1, :]


def send_out(layers, pair_rows, x, inv, kinv, turned, pick, marks, payload, spill, xcur):
    slots, wide = turned.shape[0], turned.shape[1] // LANES
    scaled = (x * kinv).astype(BF16)
    picked = jnp.dot(pick[...], scaled, preferred_element_type=F32).astype(BF16)
    group = 16
    for g in range(slots // group):
        lhs = picked[g * group : (g + 1) * group, :]
        for k in range(group):
            s = g * group + k
            got = jnp.dot(lhs, turned[s], preferred_element_type=F32)
            for w in range(wide):
                at = w * slots + s
                payload[at : at + 1, :] = got[k : k + 1, w * LANES : (w + 1) * LANES]
    meta = wide * slots
    payload[meta : meta + META, :] = marks[...]
    payload[meta + 1 : meta + 2, :] = lane_sum(x * inv)
    layer = lax.axis_index("layer")
    spread = jnp.where((layer == 0) | (layer == layers - 1), 1.0, 0.5).astype(F32) * coupling
    if x.shape[0] == pair_rows:
        own = x
    else:
        first_row = pl.multiple_of((lax.axis_index("row") // 2) * pair_rows, pair_rows)
        own = xcur[pl.ds(first_row, pair_rows), :]
    spill[...] = (own * spread).astype(BF16)


def first(layers, turned, pick, marks, *rest):
    shared, (payload, spill, xcur, inv_o, kinv_o) = rest[:-5], rest[-5:]
    slots = turned.shape[0]
    at = slots + META
    blocks = (shared[0].shape[1] - at) // 2
    if len(shared) == 1:
        parts = [(shared[0].at[r], r * blocks) for r in range(shared[0].shape[0])]
    else:
        row = lax.axis_index("row")
        starts = (row * blocks, (1 - row) * blocks)
        parts = [(ref.at[0], pl.multiple_of(at, blocks)) for ref, at in zip(shared, starts)]
    degree = None
    block_ids = lax.broadcasted_iota(jnp.int32, (xcur.shape[0], slots), 0).astype(F32)
    for ref, start in parts:
        onehot = (block_ids == ref[slots : slots + 1, 0:slots]).astype(BF16)
        part = place(onehot, ref[0:slots, :])
        degree = part if degree is None else degree + part
        mine = pl.ds(start, blocks)
        xcur[mine, :] = ref[at : at + blocks, :]
        kinv_o[mine, :] = ref[at + blocks : at + 2 * blocks, :]
    x, keep = xcur[...], kinv_o[...]
    inv = 1.0 / (keep * degree + 1.0)
    kinv = keep * inv
    inv_o[...] = inv
    kinv_o[...] = kinv
    send_out(layers, 2 * blocks, x, inv, kinv, turned, pick, marks, payload, spill, xcur)


def joined(parts):
    parts = [ref[k] for ref in parts for k in range(ref.shape[0])]
    pairs = [parts[2 * k] + parts[2 * k + 1] for k in range(len(parts) // 2)]
    return pairs[0] if len(pairs) == 1 else jnp.concatenate(pairs, axis=0)


def lane_sum(x):
    row = jnp.sum(x, axis=0, keepdims=True)
    return sum(row[:, w : w + LANES] for w in range(0, row.shape[1], LANES))


def middle(layers, turned, pick, marks, inv_i, kinv_i, xold, *rest):
    shared, (payload, spill, xcur) = rest[:-3], rest[-3:]
    x = joined(shared)
    xcur[...] = x
    send_out(layers, shared[0].shape[1], x, inv_i[...], kinv_i[...], turned, pick, marks, payload,
             spill, xcur)
    meta = payload.shape[0] - META
    payload[meta + 2 : meta + 3, :] = lane_sum(jnp.abs(x - xold[...]))


def partial(layers, node_total, early, spill, *rest):
    pays, outs = (rest[:-1], rest[-1:]) if early else (rest[:-2], rest[-2:])
    part = outs[0]
    meta, wide = pays[0].shape[0] - META, part.shape[2] // LANES
    slots = meta // wide
    blocks = part.shape[1] // 2
    odd = lax.axis_index("row") % 2
    first_block = (lax.axis_index("col") * blocks).astype(F32)
    block_ids = lax.broadcasted_iota(jnp.int32, (blocks, slots), 0).astype(F32) + first_block
    walks, sums = [], None
    for pay in pays:
        onehot = (block_ids == pay[meta : meta + 1, 0:slots]).astype(BF16)
        terms = [pay[w * slots : (w + 1) * slots, :] for w in range(wide)]
        walks.append(place(onehot, jnp.concatenate(terms, axis=1)))
        extra = pay[meta : meta + META, :]
        sums = extra if sums is None else sums + extra
    mass = jnp.sum(sums[1:2, :], axis=1, keepdims=True)
    if not early:
        outs[1][...] = sums
    end = jnp.where(odd == 0, layers - 1, 0)
    arrive = jnp.where(lax.axis_index("layer") == end, 0.0, damping * spill[...].astype(F32))
    walk = damping * (1.0 - coupling)
    own = walk * (walks[0] + mass / node_total) + (1.0 - damping)
    peer = walk * sum(walks[1:])
    part[0, 0:blocks, :] = arrive[0:blocks] + jnp.where(odd == 0, own, peer)
    part[0, blocks:, :] = arrive[blocks:] + jnp.where(odd == 0, peer, own)


def closing(xold, *rest):
    shared, (xnew, change) = rest[:-2], rest[-2:]
    x = joined(shared)
    xnew[...] = x
    change[...] = jnp.broadcast_to(lane_sum(jnp.abs(x - xold[...])), change.shape)


def flatten(xnew, ranks):
    wide = xnew.shape[1] // 128
    blocks = ranks.shape[0] // wide
    start = pl.multiple_of(lax.axis_index("row") * blocks, blocks)
    own = xnew[pl.ds(start, blocks), :]
    for w in range(wide):
        ranks[pl.ds(w, blocks, wide), :] = own[:, w * 128 : (w + 1) * 128]


def totals(*refs):
    early, late, out = refs[: ITERS - 1], refs[ITERS - 1 : -1], refs[-1]
    rows = [ref[2:3, :] for ref in early] + [sum(ref[0:1, :] for ref in late)]
    for t, row in enumerate(rows):
        out[0:1, t : t + 1] = jnp.sum(row, axis=1, keepdims=True)


def to_others(x):
    rows, cols = lax.axis_size("row"), lax.axis_size("col")
    got = []
    for step in range(1, cols):
        pairs = []
        for row in range(rows):
            for col in range(cols):
                other = (col + step) % cols if cols & (cols - 1) else col ^ step
                pairs.append((row * cols + col, (row ^ 1) * cols + other))
        got.append(lax.ppermute(x, ("row", "col"), pairs))
    return got


def to_rows(x):
    rows = lax.axis_size("row")
    if rows == 2:
        return x, lax.ppermute(x, "row", [(0, 1), (1, 0)])
    return (lax.all_gather(x, "row", axis=0, tiled=True),)


def to_layers(spill):
    layers, rows = lax.axis_size("layer"), lax.axis_size("row")
    pairs = []
    for layer in range(layers):
        for row in range(rows):
            other = layer + 1 if row % 2 == 1 else layer - 1
            here = layer * rows + row
            pairs.append((here, other * rows + row if 0 <= other < layers else layer * rows + (row ^ 1)))
    return lax.ppermute(spill, ("layer", "row"), pairs)


def local(block_values, block_rows, block_cols, block_count, dangling, start_ranks):
    slots, edge = block_values.shape[3], block_values.shape[-1]
    span = start_ranks.shape[-1]
    row_devices = lax.axis_size("row")
    layers = lax.axis_size("layer")
    node_total = row_devices * lax.axis_size("col") * span
    blocks = span // edge
    col_blk = row_devices * blocks
    flat = (span // 128, 128)
    arguments = [
        block_values.reshape(slots, edge, edge), block_cols.reshape(1, slots),
        block_rows.reshape(1, slots), block_count.reshape(1, 1), start_ranks.reshape(flat),
        dangling.reshape(flat),
    ]
    arguments = [
        x if x.size == 1 else pltpu.with_memory_space_constraint(x, pltpu.HBM) for x in arguments
    ]

    def shape(n, dtype=F32):
        return jax.ShapeDtypeStruct((n, edge), dtype)

    def lead(n):
        return jax.ShapeDtypeStruct((1, n, edge), F32)

    packed, turned, pick, marks = call(
        opening,
        (lead(slots + META + 2 * blocks), pltpu.VMEM((slots, edge, edge), BF16),
         pltpu.VMEM((slots, col_blk), BF16), pltpu.VMEM((META, LANES), F32)),
        (HBM, HBM, HBM, pl.BlockSpec(memory_space=pl.ANY), HBM, HBM),
        [pltpu.VMEM((slots, edge, edge), BF16), pltpu.VMEM((1, slots), jnp.int32),
         pltpu.VMEM((1, slots), jnp.int32), pltpu.VMEM((1, 1), jnp.int32), pltpu.VMEM(flat, F32),
         pltpu.VMEM(flat, jnp.int32), pltpu.SemaphoreType.DMA((5 + CHUNKS,))],
    )(*arguments)
    shared = to_rows(packed)
    lanes = jax.ShapeDtypeStruct((META, LANES), F32)
    products = jax.ShapeDtypeStruct((slots * edge // LANES + META, LANES), F32)
    sent = (products, shape(2 * blocks, BF16), shape(col_blk))
    payload, spill, x, inv, kinv = call(
        functools.partial(first, layers), sent + (shape(col_blk), shape(col_blk)),
        (VMEM,) * (3 + len(shared)),
    )(turned, pick, marks, *shared)
    changes = []
    for t in range(ITERS):
        if t:
            payload, spill, x = call(
                functools.partial(middle, layers), sent, (VMEM,) * (6 + len(shared)),
            )(turned, pick, marks, inv, kinv, x, *shared)
        arriving = to_layers(spill)
        others = to_others(payload)
        part, *change = call(
            functools.partial(partial, layers, node_total, t == 0),
            (lead(2 * blocks), lanes)[: 1 + (t > 0)], (VMEM,) * (2 + len(others)),
        )(arriving, payload, *others)
        changes += change
        shared = to_rows(part)
    xnew, last = call(closing, (shape(col_blk), lanes), (VMEM,) * (1 + len(shared)))(x, *shared)
    lates = [last] + to_others(last)
    ranks = call(flatten, jax.ShapeDtypeStruct(flat, F32), (VMEM,))(xnew)
    residuals = call(
        totals, jax.ShapeDtypeStruct((1, ITERS), F32),
        (VMEM,) * (ITERS - 1 + len(lates)),
    )(*changes, *lates)
    return ranks.reshape(start_ranks.shape), residuals.reshape(ITERS, 1)


def solution(mesh):
    placed = (
        P("layer", "row", "col", None, None, None),
        P("layer", "row", "col", None),
        P("layer", "row", "col", None),
        P("layer", "row", "col"),
        P("layer", "row", "col", None),
        P("layer", "row", "col", None),
    )
    return jax.shard_map(
        local,
        mesh=mesh,
        in_specs=placed,
        out_specs=(P("layer", "row", "col", None), P(None, "layer")),
        check_vma=False,
    )
```

```python
import functools
import jax
import jax.numpy as jnp
from jax import lax
from jax.experimental import pallas as pl
from jax.experimental.pallas import tpu as pltpu
from jax.sharding import PartitionSpec as P

ITERS = 3
damping = 0.85
coupling = 0.3

F32 = jnp.float32
BF16 = jnp.bfloat16
VMEM = pl.BlockSpec(memory_space=pltpu.VMEM)
HBM = pl.BlockSpec(memory_space=pltpu.HBM)
META = 8
LANES = 128
CHUNKS = 4


def call(body, outs, specs, scratch=(), aliases={}):
    return pl.pallas_call(
        body,
        out_shape=outs,
        in_specs=specs,
        out_specs=(VMEM,) * len(outs) if isinstance(outs, tuple) else VMEM,
        scratch_shapes=scratch,
        input_output_aliases=aliases,
        compiler_params=pltpu.CompilerParams(vmem_limit_bytes=24 * 1024 * 1024),
    )


def two_terms(x):
    hi = x.astype(BF16)
    return hi, (x - hi.astype(F32)).astype(BF16)


def place(onehot, rows):
    hi, lo = two_terms(rows)
    return jnp.dot(onehot, hi, preferred_element_type=F32) + jnp.dot(
        onehot, lo, preferred_element_type=F32
    )


def to_blocks(ref, edge):
    wide = edge // 128
    count = ref.shape[0] // wide
    return jnp.concatenate([ref[pl.ds(w, count, wide), :] for w in range(wide)], axis=1)


def opening(values_h, cols_h, rows_h, count_h, x_h, dangling_h, packed, turned, pick, marks,
            values, cols, rows, count, x, dangling, sems):
    slots, edge, _ = values.shape
    blocks = x.shape[0] * 128 // edge
    step = slots // CHUNKS
    large = [
        pltpu.make_async_copy(
            values_h.at[pl.ds(k * step, step)], values.at[pl.ds(k * step, step)], sems.at[k]
        )
        for k in range(CHUNKS)
    ]
    pairs = ((cols_h, cols), (rows_h, rows), (count_h, count), (x_h, x), (dangling_h, dangling))
    small = [
        pltpu.make_async_copy(source, target, sems.at[CHUNKS + k])
        for k, (source, target) in enumerate(pairs)
    ]
    for copy in small + large:
        copy.start()
    for copy in small:
        copy.wait()
    live = lax.broadcasted_iota(jnp.int32, (1, slots), 1) < count[...]
    packed[0, slots : slots + META, :] = jnp.zeros((META, edge), F32)
    packed[0, slots : slots + 1, 0:slots] = jnp.where(live, cols[...], -1).astype(F32)
    marks[...] = jnp.zeros((META, LANES), F32)
    marks[0:1, 0:slots] = jnp.where(live, rows[...], -1).astype(F32)
    source_ids = lax.broadcasted_iota(jnp.int32, (pick.shape[1], slots), 0)
    pick[...] = (source_ids == cols[...]).astype(F32).T.astype(BF16)
    at = slots + META
    packed[0, at : at + blocks, :] = to_blocks(x, edge)
    packed[0, at + blocks : at + 2 * blocks, :] = 1.0 - to_blocks(dangling, edge).astype(F32)
    ones = jnp.ones((16, edge), BF16)
    for k in range(CHUNKS):
        large[k].wait()
        for s in range(k * step, (k + 1) * step):
            block = values[s]
            turned[s] = block.T
            got = jnp.dot(ones, block, preferred_element_type=F32)
            packed[0, s : s + 1, :] = got[0:1, :]


def send_out(layers, pair_rows, x, inv, kinv, turned, pick, marks, payload, spill, xcur):
    slots, wide = turned.shape[0], turned.shape[1] // LANES
    scaled = (x * kinv).astype(BF16)
    picked = jnp.dot(pick[...], scaled, preferred_element_type=F32).astype(BF16)
    group = 16
    for g in range(slots // group):
        lhs = picked[g * group : (g + 1) * group, :]
        for k in range(group):
            s = g * group + k
            got = jnp.dot(lhs, turned[s], preferred_element_type=F32)
            for w in range(wide):
                at = w * slots + s
                payload[at : at + 1, :] = got[k : k + 1, w * LANES : (w + 1) * LANES]
    meta = wide * slots
    payload[meta : meta + META, :] = marks[...]
    payload[meta + 1 : meta + 2, :] = lane_sum(x * inv)
    layer = lax.axis_index("layer")
    spread = jnp.where((layer == 0) | (layer == layers - 1), 1.0, 0.5).astype(F32) * coupling
    if x.shape[0] == pair_rows:
        own = x
    else:
        first_row = pl.multiple_of((lax.axis_index("row") // 2) * pair_rows, pair_rows)
        own = xcur[pl.ds(first_row, pair_rows), :]
    spill[...] = (own * spread).astype(BF16)


def first(layers, turned, pick, marks, *rest):
    shared, (payload, spill, xcur, inv_o, kinv_o) = rest[:-5], rest[-5:]
    slots = turned.shape[0]
    at = slots + META
    blocks = (shared[0].shape[1] - at) // 2
    if len(shared) == 1:
        parts = [(shared[0].at[r], r * blocks) for r in range(shared[0].shape[0])]
    else:
        row = lax.axis_index("row")
        starts = (row * blocks, (1 - row) * blocks)
        parts = [(ref.at[0], pl.multiple_of(at, blocks)) for ref, at in zip(shared, starts)]
    degree = None
    block_ids = lax.broadcasted_iota(jnp.int32, (xcur.shape[0], slots), 0).astype(F32)
    for ref, start in parts:
        onehot = (block_ids == ref[slots : slots + 1, 0:slots]).astype(BF16)
        part = place(onehot, ref[0:slots, :])
        degree = part if degree is None else degree + part
        mine = pl.ds(start, blocks)
        xcur[mine, :] = ref[at : at + blocks, :]
        kinv_o[mine, :] = ref[at + blocks : at + 2 * blocks, :]
    x, keep = xcur[...], kinv_o[...]
    inv = 1.0 / (keep * degree + 1.0)
    kinv = keep * inv
    inv_o[...] = inv
    kinv_o[...] = kinv
    send_out(layers, 2 * blocks, x, inv, kinv, turned, pick, marks, payload, spill, xcur)


def joined(parts):
    parts = [ref[k] for ref in parts for k in range(ref.shape[0])]
    pairs = [parts[2 * k] + parts[2 * k + 1] for k in range(len(parts) // 2)]
    return pairs[0] if len(pairs) == 1 else jnp.concatenate(pairs, axis=0)


def lane_sum(x):
    row = jnp.sum(x, axis=0, keepdims=True)
    return sum(row[:, w : w + LANES] for w in range(0, row.shape[1], LANES))


def middle(layers, turned, pick, marks, inv_i, kinv_i, xold, *rest):
    shared, (payload, spill, xcur) = rest[:-3], rest[-3:]
    x = joined(shared)
    xcur[...] = x
    send_out(layers, shared[0].shape[1], x, inv_i[...], kinv_i[...], turned, pick, marks, payload,
             spill, xcur)
    meta = payload.shape[0] - META
    payload[meta + 2 : meta + 3, :] = lane_sum(jnp.abs(x - xold[...]))


def partial(layers, node_total, early, spill, *rest):
    pays, outs = (rest[:-1], rest[-1:]) if early else (rest[:-2], rest[-2:])
    part = outs[0]
    meta, wide = pays[0].shape[0] - META, part.shape[2] // LANES
    slots = meta // wide
    blocks = part.shape[1] // 2
    odd = lax.axis_index("row") % 2
    first_block = (lax.axis_index("col") * blocks).astype(F32)
    block_ids = lax.broadcasted_iota(jnp.int32, (blocks, slots), 0).astype(F32) + first_block
    walks, sums = [], None
    for pay in pays:
        onehot = (block_ids == pay[meta : meta + 1, 0:slots]).astype(BF16)
        terms = [pay[w * slots : (w + 1) * slots, :] for w in range(wide)]
        walks.append(place(onehot, jnp.concatenate(terms, axis=1)))
        extra = pay[meta : meta + META, :]
        sums = extra if sums is None else sums + extra
    mass = jnp.sum(sums[1:2, :], axis=1, keepdims=True)
    if not early:
        outs[1][...] = sums
    end = jnp.where(odd == 0, layers - 1, 0)
    arrive = jnp.where(lax.axis_index("layer") == end, 0.0, damping * spill[...].astype(F32))
    walk = damping * (1.0 - coupling)
    own = walk * (sum(walks[:2]) + mass / node_total) + (1.0 - damping)
    peer = walk * sum(walks[2:])
    part[0, 0:blocks, :] = arrive[0:blocks] + jnp.where(odd == 0, own, peer)
    part[0, blocks:, :] = arrive[blocks:] + jnp.where(odd == 0, peer, own)


def closing(xold, *rest):
    shared, (xnew, change) = rest[:-2], rest[-2:]
    x = joined(shared)
    xnew[...] = x
    change[...] = jnp.broadcast_to(lane_sum(jnp.abs(x - xold[...])), change.shape)


def flatten(xnew, ranks):
    wide = xnew.shape[1] // 128
    blocks = ranks.shape[0] // wide
    start = pl.multiple_of(lax.axis_index("row") * blocks, blocks)
    own = xnew[pl.ds(start, blocks), :]
    for w in range(wide):
        ranks[pl.ds(w, blocks, wide), :] = own[:, w * 128 : (w + 1) * 128]


def totals(*refs):
    early, late, out = refs[: ITERS - 1], refs[ITERS - 1 : -1], refs[-1]
    rows = [ref[2:3, :] for ref in early] + [sum(ref[0:1, :] for ref in late)]
    for t, row in enumerate(rows):
        out[0:1, t : t + 1] = jnp.sum(row, axis=1, keepdims=True)


def to_others(x):
    rows, cols = lax.axis_size("row"), lax.axis_size("col")
    got = []
    for step in range(1, cols):
        pairs = []
        for row in range(rows):
            for col in range(cols):
                other = (col + step) % cols if cols & (cols - 1) else col ^ step
                pairs.append((row * cols + col, (row ^ (step > 1)) * cols + other))
        got.append(lax.ppermute(x, ("row", "col"), pairs))
    return got


def to_rows(x):
    rows = lax.axis_size("row")
    if rows == 2:
        return x, lax.ppermute(x, "row", [(0, 1), (1, 0)])
    return (lax.all_gather(x, "row", axis=0, tiled=True),)


def to_layers(spill):
    layers, rows = lax.axis_size("layer"), lax.axis_size("row")
    pairs = []
    for layer in range(layers):
        for row in range(rows):
            other = layer + 1 if row % 2 == 1 else layer - 1
            here = layer * rows + row
            pairs.append((here, other * rows + row if 0 <= other < layers else layer * rows + (row ^ 1)))
    return lax.ppermute(spill, ("layer", "row"), pairs)


def local(block_values, block_rows, block_cols, block_count, dangling, start_ranks):
    slots, edge = block_values.shape[3], block_values.shape[-1]
    span = start_ranks.shape[-1]
    row_devices = lax.axis_size("row")
    layers = lax.axis_size("layer")
    node_total = row_devices * lax.axis_size("col") * span
    blocks = span // edge
    col_blk = row_devices * blocks
    flat = (span // 128, 128)
    arguments = [
        block_values.reshape(slots, edge, edge), block_cols.reshape(1, slots),
        block_rows.reshape(1, slots), block_count.reshape(1, 1), start_ranks.reshape(flat),
        dangling.reshape(flat),
    ]
    arguments = [
        x if x.size == 1 else pltpu.with_memory_space_constraint(x, pltpu.HBM) for x in arguments
    ]

    def shape(n, dtype=F32):
        return jax.ShapeDtypeStruct((n, edge), dtype)

    def lead(n):
        return jax.ShapeDtypeStruct((1, n, edge), F32)

    packed, turned, pick, marks = call(
        opening,
        (lead(slots + META + 2 * blocks), pltpu.VMEM((slots, edge, edge), BF16),
         pltpu.VMEM((slots, col_blk), BF16), pltpu.VMEM((META, LANES), F32)),
        (HBM, HBM, HBM, pl.BlockSpec(memory_space=pl.ANY), HBM, HBM),
        [pltpu.VMEM((slots, edge, edge), BF16), pltpu.VMEM((1, slots), jnp.int32),
         pltpu.VMEM((1, slots), jnp.int32), pltpu.VMEM((1, 1), jnp.int32), pltpu.VMEM(flat, F32),
         pltpu.VMEM(flat, jnp.int32), pltpu.SemaphoreType.DMA((5 + CHUNKS,))],
    )(*arguments)
    shared = to_rows(packed)
    lanes = jax.ShapeDtypeStruct((META, LANES), F32)
    products = jax.ShapeDtypeStruct((slots * edge // LANES + META, LANES), F32)
    sent = (products, shape(2 * blocks, BF16), shape(col_blk))
    payload, spill, x, inv, kinv = call(
        functools.partial(first, layers), sent + (shape(col_blk), shape(col_blk)),
        (VMEM,) * (3 + len(shared)),
    )(turned, pick, marks, *shared)
    changes = []
    for t in range(ITERS):
        if t:
            payload, spill, x = call(
                functools.partial(middle, layers), sent, (VMEM,) * (6 + len(shared)),
            )(turned, pick, marks, inv, kinv, x, *shared)
        arriving = to_layers(spill)
        others = to_others(payload)
        part, *change = call(
            functools.partial(partial, layers, node_total, t == 0),
            (lead(2 * blocks), lanes)[: 1 + (t > 0)], (VMEM,) * (2 + len(others)),
        )(arriving, payload, *others)
        changes += change
        shared = to_rows(part)
    xnew, last = call(closing, (shape(col_blk), lanes), (VMEM,) * (1 + len(shared)))(x, *shared)
    lates = [last] + to_others(last)
    ranks = call(flatten, jax.ShapeDtypeStruct(flat, F32), (VMEM,))(xnew)
    residuals = call(
        totals, jax.ShapeDtypeStruct((1, ITERS), F32),
        (VMEM,) * (ITERS - 1 + len(lates)),
    )(*changes, *lates)
    return ranks.reshape(start_ranks.shape), residuals.reshape(ITERS, 1)


def solution(mesh):
    placed = (
        P("layer", "row", "col", None, None, None),
        P("layer", "row", "col", None),
        P("layer", "row", "col", None),
        P("layer", "row", "col"),
        P("layer", "row", "col", None),
        P("layer", "row", "col", None),
    )
    return jax.shard_map(
        local,
        mesh=mesh,
        in_specs=placed,
        out_specs=(P("layer", "row", "col", None), P(None, "layer")),
        check_vma=False,
    )
```

```python
import functools
import jax
import jax.numpy as jnp
from jax import lax
from jax.experimental import pallas as pl
from jax.experimental.pallas import tpu as pltpu
from jax.sharding import PartitionSpec as P

ITERS = 3
damping = 0.85
coupling = 0.3

F32 = jnp.float32
BF16 = jnp.bfloat16
VMEM = pl.BlockSpec(memory_space=pltpu.VMEM)
HBM = pl.BlockSpec(memory_space=pltpu.HBM)
META = 8
LANES = 128
CHUNKS = 4


def call(body, outs, specs, scratch=(), aliases={}):
    return pl.pallas_call(
        body,
        out_shape=outs,
        in_specs=specs,
        out_specs=(VMEM,) * len(outs) if isinstance(outs, tuple) else VMEM,
        scratch_shapes=scratch,
        input_output_aliases=aliases,
        compiler_params=pltpu.CompilerParams(vmem_limit_bytes=24 * 1024 * 1024),
    )


def two_terms(x):
    hi = x.astype(BF16)
    return hi, (x - hi.astype(F32)).astype(BF16)


def place(onehot, rows):
    hi, lo = two_terms(rows)
    return jnp.dot(onehot, hi, preferred_element_type=F32) + jnp.dot(
        onehot, lo, preferred_element_type=F32
    )


def to_blocks(ref, edge):
    wide = edge // 128
    count = ref.shape[0] // wide
    return jnp.concatenate([ref[pl.ds(w, count, wide), :] for w in range(wide)], axis=1)


def opening(values_h, cols_h, rows_h, count_h, x_h, dangling_h, packed, values, pick, marks,
            cols, rows, count, x, dangling, sems):
    slots, edge, _ = values.shape
    blocks = x.shape[0] * 128 // edge
    step = slots // CHUNKS
    large = [
        pltpu.make_async_copy(
            values_h.at[pl.ds(k * step, step)], values.at[pl.ds(k * step, step)], sems.at[k]
        )
        for k in range(CHUNKS)
    ]
    pairs = ((cols_h, cols), (rows_h, rows), (count_h, count), (x_h, x), (dangling_h, dangling))
    small = [
        pltpu.make_async_copy(source, target, sems.at[CHUNKS + k])
        for k, (source, target) in enumerate(pairs)
    ]
    for copy in small + large:
        copy.start()
    for copy in small:
        copy.wait()
    live = lax.broadcasted_iota(jnp.int32, (1, slots), 1) < count[...]
    packed[0, slots : slots + META, :] = jnp.zeros((META, edge), F32)
    packed[0, slots : slots + 1, 0:slots] = jnp.where(live, cols[...], -1).astype(F32)
    marks[...] = jnp.zeros((META, LANES), F32)
    marks[0:1, 0:slots] = jnp.where(live, rows[...], -1).astype(F32)
    source_ids = lax.broadcasted_iota(jnp.int32, (pick.shape[1], slots), 0)
    pick[...] = (source_ids == cols[...]).astype(F32).T.astype(BF16)
    at = slots + META
    packed[0, at : at + blocks, :] = to_blocks(x, edge)
    packed[0, at + blocks : at + 2 * blocks, :] = 1.0 - to_blocks(dangling, edge).astype(F32)
    ones = jnp.ones((16, edge), BF16)
    for k in range(CHUNKS):
        large[k].wait()
        for s in range(k * step, (k + 1) * step):
            block = values[s]
            got = jnp.dot(ones, block, preferred_element_type=F32)
            packed[0, s : s + 1, :] = got[0:1, :]


def turn(values, turned):
    for s in range(values.shape[0]):
        turned[s] = values[s].T


def send_out(layers, pair_rows, x, inv, kinv, turned, pick, marks, payload, spill, xcur):
    slots, wide = turned.shape[0], turned.shape[1] // LANES
    scaled = (x * kinv).astype(BF16)
    picked = jnp.dot(pick[...], scaled, preferred_element_type=F32).astype(BF16)
    group = 16
    for g in range(slots // group):
        lhs = picked[g * group : (g + 1) * group, :]
        for k in range(group):
            s = g * group + k
            got = jnp.dot(lhs, turned[s], preferred_element_type=F32)
            for w in range(wide):
                at = w * slots + s
                payload[at : at + 1, :] = got[k : k + 1, w * LANES : (w + 1) * LANES]
    meta = wide * slots
    payload[meta : meta + META, :] = marks[...]
    payload[meta + 1 : meta + 2, :] = lane_sum(x * inv)
    layer = lax.axis_index("layer")
    spread = jnp.where((layer == 0) | (layer == layers - 1), 1.0, 0.5).astype(F32) * coupling
    if x.shape[0] == pair_rows:
        own = x
    else:
        first_row = pl.multiple_of((lax.axis_index("row") // 2) * pair_rows, pair_rows)
        own = xcur[pl.ds(first_row, pair_rows), :]
    spill[...] = (own * spread).astype(BF16)


def first(layers, turned, pick, marks, *rest):
    shared, (payload, spill, xcur, inv_o, kinv_o) = rest[:-5], rest[-5:]
    slots = turned.shape[0]
    at = slots + META
    blocks = (shared[0].shape[1] - at) // 2
    if len(shared) == 1:
        parts = [(shared[0].at[r], r * blocks) for r in range(shared[0].shape[0])]
    else:
        row = lax.axis_index("row")
        starts = (row * blocks, (1 - row) * blocks)
        parts = [(ref.at[0], pl.multiple_of(at, blocks)) for ref, at in zip(shared, starts)]
    degree = None
    block_ids = lax.broadcasted_iota(jnp.int32, (xcur.shape[0], slots), 0).astype(F32)
    for ref, start in parts:
        onehot = (block_ids == ref[slots : slots + 1, 0:slots]).astype(BF16)
        part = place(onehot, ref[0:slots, :])
        degree = part if degree is None else degree + part
        mine = pl.ds(start, blocks)
        xcur[mine, :] = ref[at : at + blocks, :]
        kinv_o[mine, :] = ref[at + blocks : at + 2 * blocks, :]
    x, keep = xcur[...], kinv_o[...]
    inv = 1.0 / (keep * degree + 1.0)
    kinv = keep * inv
    inv_o[...] = inv
    kinv_o[...] = kinv
    send_out(layers, 2 * blocks, x, inv, kinv, turned, pick, marks, payload, spill, xcur)


def joined(parts):
    parts = [ref[k] for ref in parts for k in range(ref.shape[0])]
    pairs = [parts[2 * k] + parts[2 * k + 1] for k in range(len(parts) // 2)]
    return pairs[0] if len(pairs) == 1 else jnp.concatenate(pairs, axis=0)


def lane_sum(x):
    row = jnp.sum(x, axis=0, keepdims=True)
    return sum(row[:, w : w + LANES] for w in range(0, row.shape[1], LANES))


def middle(layers, turned, pick, marks, inv_i, kinv_i, xold, *rest):
    shared, (payload, spill, xcur) = rest[:-3], rest[-3:]
    x = joined(shared)
    xcur[...] = x
    send_out(layers, shared[0].shape[1], x, inv_i[...], kinv_i[...], turned, pick, marks, payload,
             spill, xcur)
    meta = payload.shape[0] - META
    payload[meta + 2 : meta + 3, :] = lane_sum(jnp.abs(x - xold[...]))


def partial(layers, node_total, early, spill, *rest):
    pays, outs = (rest[:-1], rest[-1:]) if early else (rest[:-2], rest[-2:])
    part = outs[0]
    meta, wide = pays[0].shape[0] - META, part.shape[2] // LANES
    slots = meta // wide
    blocks = part.shape[1] // 2
    odd = lax.axis_index("row") % 2
    first_block = (lax.axis_index("col") * blocks).astype(F32)
    block_ids = lax.broadcasted_iota(jnp.int32, (blocks, slots), 0).astype(F32) + first_block
    walks, sums = [], None
    for pay in pays:
        onehot = (block_ids == pay[meta : meta + 1, 0:slots]).astype(BF16)
        terms = [pay[w * slots : (w + 1) * slots, :] for w in range(wide)]
        walks.append(place(onehot, jnp.concatenate(terms, axis=1)))
        extra = pay[meta : meta + META, :]
        sums = extra if sums is None else sums + extra
    mass = jnp.sum(sums[1:2, :], axis=1, keepdims=True)
    if not early:
        outs[1][...] = sums
    end = jnp.where(odd == 0, layers - 1, 0)
    arrive = jnp.where(lax.axis_index("layer") == end, 0.0, damping * spill[...].astype(F32))
    walk = damping * (1.0 - coupling)
    own = walk * (sum(walks[:2]) + mass / node_total) + (1.0 - damping)
    peer = walk * sum(walks[2:])
    part[0, 0:blocks, :] = arrive[0:blocks] + jnp.where(odd == 0, own, peer)
    part[0, blocks:, :] = arrive[blocks:] + jnp.where(odd == 0, peer, own)


def closing(xold, *rest):
    shared, (xnew, change) = rest[:-2], rest[-2:]
    x = joined(shared)
    xnew[...] = x
    change[...] = jnp.broadcast_to(lane_sum(jnp.abs(x - xold[...])), change.shape)


def flatten(xnew, ranks):
    wide = xnew.shape[1] // 128
    blocks = ranks.shape[0] // wide
    start = pl.multiple_of(lax.axis_index("row") * blocks, blocks)
    own = xnew[pl.ds(start, blocks), :]
    for w in range(wide):
        ranks[pl.ds(w, blocks, wide), :] = own[:, w * 128 : (w + 1) * 128]


def totals(*refs):
    early, late, out = refs[: ITERS - 1], refs[ITERS - 1 : -1], refs[-1]
    rows = [ref[2:3, :] for ref in early] + [sum(ref[0:1, :] for ref in late)]
    for t, row in enumerate(rows):
        out[0:1, t : t + 1] = jnp.sum(row, axis=1, keepdims=True)


def to_others(x):
    rows, cols = lax.axis_size("row"), lax.axis_size("col")
    got = []
    for step in range(1, cols):
        pairs = []
        for row in range(rows):
            for col in range(cols):
                other = (col + step) % cols if cols & (cols - 1) else col ^ step
                pairs.append((row * cols + col, (row ^ (step > 1)) * cols + other))
        got.append(lax.ppermute(x, ("row", "col"), pairs))
    return got


def to_rows(x):
    rows = lax.axis_size("row")
    if rows == 2:
        return x, lax.ppermute(x, "row", [(0, 1), (1, 0)])
    return (lax.all_gather(x, "row", axis=0, tiled=True),)


def to_layers(spill):
    layers, rows = lax.axis_size("layer"), lax.axis_size("row")
    pairs = []
    for layer in range(layers):
        for row in range(rows):
            other = layer + 1 if row % 2 == 1 else layer - 1
            here = layer * rows + row
            pairs.append((here, other * rows + row if 0 <= other < layers else layer * rows + (row ^ 1)))
    return lax.ppermute(spill, ("layer", "row"), pairs)


def local(block_values, block_rows, block_cols, block_count, dangling, start_ranks):
    slots, edge = block_values.shape[3], block_values.shape[-1]
    span = start_ranks.shape[-1]
    row_devices = lax.axis_size("row")
    layers = lax.axis_size("layer")
    node_total = row_devices * lax.axis_size("col") * span
    blocks = span // edge
    col_blk = row_devices * blocks
    flat = (span // 128, 128)
    arguments = [
        block_values.reshape(slots, edge, edge), block_cols.reshape(1, slots),
        block_rows.reshape(1, slots), block_count.reshape(1, 1), start_ranks.reshape(flat),
        dangling.reshape(flat),
    ]
    arguments = [
        x if x.size == 1 else pltpu.with_memory_space_constraint(x, pltpu.HBM) for x in arguments
    ]

    def shape(n, dtype=F32):
        return jax.ShapeDtypeStruct((n, edge), dtype)

    def lead(n):
        return jax.ShapeDtypeStruct((1, n, edge), F32)

    packed, values, pick, marks = call(
        opening,
        (lead(slots + META + 2 * blocks), pltpu.VMEM((slots, edge, edge), BF16),
         pltpu.VMEM((slots, col_blk), BF16), pltpu.VMEM((META, LANES), F32)),
        (HBM, HBM, HBM, pl.BlockSpec(memory_space=pl.ANY), HBM, HBM),
        [pltpu.VMEM((1, slots), jnp.int32),
         pltpu.VMEM((1, slots), jnp.int32), pltpu.VMEM((1, 1), jnp.int32), pltpu.VMEM(flat, F32),
         pltpu.VMEM(flat, jnp.int32), pltpu.SemaphoreType.DMA((5 + CHUNKS,))],
    )(*arguments)
    shared = to_rows(packed)
    turned = call(turn, pltpu.VMEM((slots, edge, edge), BF16), (VMEM,))(values)
    lanes = jax.ShapeDtypeStruct((META, LANES), F32)
    products = jax.ShapeDtypeStruct((slots * edge // LANES + META, LANES), F32)
    sent = (products, shape(2 * blocks, BF16), shape(col_blk))
    payload, spill, x, inv, kinv = call(
        functools.partial(first, layers), sent + (shape(col_blk), shape(col_blk)),
        (VMEM,) * (3 + len(shared)),
    )(turned, pick, marks, *shared)
    changes = []
    for t in range(ITERS):
        if t:
            payload, spill, x = call(
                functools.partial(middle, layers), sent, (VMEM,) * (6 + len(shared)),
            )(turned, pick, marks, inv, kinv, x, *shared)
        arriving = to_layers(spill)
        others = to_others(payload)
        part, *change = call(
            functools.partial(partial, layers, node_total, t == 0),
            (lead(2 * blocks), lanes)[: 1 + (t > 0)], (VMEM,) * (2 + len(others)),
        )(arriving, payload, *others)
        changes += change
        shared = to_rows(part)
    xnew, last = call(closing, (shape(col_blk), lanes), (VMEM,) * (1 + len(shared)))(x, *shared)
    lates = [last] + to_others(last)
    ranks = call(flatten, jax.ShapeDtypeStruct(flat, F32), (VMEM,))(xnew)
    residuals = call(
        totals, jax.ShapeDtypeStruct((1, ITERS), F32),
        (VMEM,) * (ITERS - 1 + len(lates)),
    )(*changes, *lates)
    return ranks.reshape(start_ranks.shape), residuals.reshape(ITERS, 1)


def solution(mesh):
    placed = (
        P("layer", "row", "col", None, None, None),
        P("layer", "row", "col", None),
        P("layer", "row", "col", None),
        P("layer", "row", "col"),
        P("layer", "row", "col", None),
        P("layer", "row", "col", None),
    )
    return jax.shard_map(
        local,
        mesh=mesh,
        in_specs=placed,
        out_specs=(P("layer", "row", "col", None), P(None, "layer")),
        check_vma=False,
    )
```

```python
import functools
import jax
import jax.numpy as jnp
from jax import lax
from jax.experimental import pallas as pl
from jax.experimental.pallas import tpu as pltpu
from jax.sharding import PartitionSpec as P

ITERS = 3
damping = 0.85
coupling = 0.3

F32 = jnp.float32
BF16 = jnp.bfloat16
VMEM = pl.BlockSpec(memory_space=pltpu.VMEM)
HBM = pl.BlockSpec(memory_space=pltpu.HBM)
META = 8
LANES = 128
CHUNKS = 4


def call(body, outs, specs, scratch=(), aliases={}):
    return pl.pallas_call(
        body,
        out_shape=outs,
        in_specs=specs,
        out_specs=(VMEM,) * len(outs) if isinstance(outs, tuple) else VMEM,
        scratch_shapes=scratch,
        input_output_aliases=aliases,
        compiler_params=pltpu.CompilerParams(vmem_limit_bytes=24 * 1024 * 1024),
    )


def two_terms(x):
    hi = x.astype(BF16)
    return hi, (x - hi.astype(F32)).astype(BF16)


def place(onehot, rows):
    hi, lo = two_terms(rows)
    return jnp.dot(onehot, hi, preferred_element_type=F32) + jnp.dot(
        onehot, lo, preferred_element_type=F32
    )


def tree(terms):
    while len(terms) > 1:
        terms = [sum(terms[k + 1 : k + 2], terms[k]) for k in range(0, len(terms), 2)]
    return terms[0]


def to_blocks(ref, edge):
    wide = edge // 128
    count = ref.shape[0] // wide
    return jnp.concatenate([ref[pl.ds(w, count, wide), :] for w in range(wide)], axis=1)


def opening(values_h, cols_h, rows_h, count_h, x_h, dangling_h, packed, values, pick, marks,
            cols, rows, count, x, dangling, sems):
    slots, edge, _ = values.shape
    blocks = x.shape[0] * 128 // edge
    step = slots // CHUNKS
    large = [
        pltpu.make_async_copy(
            values_h.at[pl.ds(k * step, step)], values.at[pl.ds(k * step, step)], sems.at[k]
        )
        for k in range(CHUNKS)
    ]
    pairs = ((cols_h, cols), (rows_h, rows), (count_h, count), (x_h, x), (dangling_h, dangling))
    small = [
        pltpu.make_async_copy(source, target, sems.at[CHUNKS + k])
        for k, (source, target) in enumerate(pairs)
    ]
    for copy in small + large:
        copy.start()
    for copy in small:
        copy.wait()
    live = lax.broadcasted_iota(jnp.int32, (1, slots), 1) < count[...]
    packed[0, slots : slots + META, :] = jnp.zeros((META, edge), F32)
    packed[0, slots : slots + 1, 0:slots] = jnp.where(live, cols[...], -1).astype(F32)
    marks[...] = jnp.zeros((META, LANES), F32)
    marks[0:1, 0:slots] = jnp.where(live, rows[...], -1).astype(F32)
    source_ids = lax.broadcasted_iota(jnp.int32, (pick.shape[1], slots), 0)
    pick[...] = (source_ids == cols[...]).astype(F32).T.astype(BF16)
    at = slots + META
    packed[0, at : at + blocks, :] = to_blocks(x, edge)
    packed[0, at + blocks : at + 2 * blocks, :] = 1.0 - to_blocks(dangling, edge).astype(F32)
    ones = jnp.ones((16, edge), BF16)
    for k in range(CHUNKS):
        large[k].wait()
        for s in range(k * step, (k + 1) * step):
            block = values[s]
            got = jnp.dot(ones, block, preferred_element_type=F32)
            packed[0, s : s + 1, :] = got[0:1, :]


def turn(values, turned):
    for s in range(values.shape[0]):
        turned[s] = values[s].T


def send_out(layers, pair_rows, x, inv, kinv, turned, pick, marks, payload, spill, xcur):
    slots, wide = turned.shape[0], turned.shape[1] // LANES
    scaled = (x * kinv).astype(BF16)
    picked = jnp.dot(pick[...], scaled, preferred_element_type=F32).astype(BF16)
    group = 16
    for g in range(slots // group):
        lhs = picked[g * group : (g + 1) * group, :]
        for k in range(group):
            s = g * group + k
            got = jnp.dot(lhs, turned[s], preferred_element_type=F32)
            for w in range(wide):
                at = w * slots + s
                payload[at : at + 1, :] = got[k : k + 1, w * LANES : (w + 1) * LANES]
    meta = wide * slots
    payload[meta : meta + META, :] = marks[...]
    payload[meta + 1 : meta + 2, :] = lane_sum(x * inv)
    layer = lax.axis_index("layer")
    spread = jnp.where((layer == 0) | (layer == layers - 1), 1.0, 0.5).astype(F32) * coupling
    if x.shape[0] == pair_rows:
        own = x
    else:
        first_row = pl.multiple_of((lax.axis_index("row") // 2) * pair_rows, pair_rows)
        own = xcur[pl.ds(first_row, pair_rows), :]
    spill[...] = (own * spread).astype(BF16)


def first(layers, turned, pick, marks, *rest):
    shared, (payload, spill, xcur, inv_o, kinv_o) = rest[:-5], rest[-5:]
    slots = turned.shape[0]
    at = slots + META
    blocks = (shared[0].shape[1] - at) // 2
    if len(shared) == 1:
        parts = [(shared[0].at[r], r * blocks) for r in range(shared[0].shape[0])]
    else:
        row = lax.axis_index("row")
        starts = (row * blocks, (1 - row) * blocks)
        parts = [(ref.at[0], pl.multiple_of(at, blocks)) for ref, at in zip(shared, starts)]
    degree = None
    block_ids = lax.broadcasted_iota(jnp.int32, (xcur.shape[0], slots), 0).astype(F32)
    for ref, start in parts:
        onehot = (block_ids == ref[slots : slots + 1, 0:slots]).astype(BF16)
        part = place(onehot, ref[0:slots, :])
        degree = part if degree is None else degree + part
        mine = pl.ds(start, blocks)
        xcur[mine, :] = ref[at : at + blocks, :]
        kinv_o[mine, :] = ref[at + blocks : at + 2 * blocks, :]
    x, keep = xcur[...], kinv_o[...]
    inv = 1.0 / (keep * degree + 1.0)
    kinv = keep * inv
    inv_o[...] = inv
    kinv_o[...] = kinv
    send_out(layers, 2 * blocks, x, inv, kinv, turned, pick, marks, payload, spill, xcur)


def joined(parts):
    parts = [ref[k] for ref in parts for k in range(ref.shape[0])]
    pairs = [parts[2 * k] + parts[2 * k + 1] for k in range(len(parts) // 2)]
    return pairs[0] if len(pairs) == 1 else jnp.concatenate(pairs, axis=0)


def lane_sum(x):
    row = jnp.sum(x, axis=0, keepdims=True)
    return sum(row[:, w : w + LANES] for w in range(0, row.shape[1], LANES))


def middle(layers, turned, pick, marks, inv_i, kinv_i, xold, *rest):
    shared, (payload, spill, xcur) = rest[:-3], rest[-3:]
    x = joined(shared)
    xcur[...] = x
    send_out(layers, shared[0].shape[1], x, inv_i[...], kinv_i[...], turned, pick, marks, payload,
             spill, xcur)
    meta = payload.shape[0] - META
    payload[meta + 2 : meta + 3, :] = lane_sum(jnp.abs(x - xold[...]))


def partial(layers, node_total, early, spill, *rest):
    pays, outs = (rest[:-1], rest[-1:]) if early else (rest[:-2], rest[-2:])
    part = outs[0]
    meta, wide = pays[0].shape[0] - META, part.shape[2] // LANES
    slots = meta // wide
    blocks = part.shape[1] // 2
    odd = lax.axis_index("row") % 2
    first_block = (lax.axis_index("col") * blocks).astype(F32)
    block_ids = lax.broadcasted_iota(jnp.int32, (blocks, slots), 0).astype(F32) + first_block
    walks, extras = [], []
    for pay in pays:
        onehot = (block_ids == pay[meta : meta + 1, 0:slots]).astype(BF16)
        terms = [pay[w * slots : (w + 1) * slots, :] for w in range(wide)]
        walks.append(place(onehot, jnp.concatenate(terms, axis=1)))
        extras.append(pay[meta : meta + META, :])
    sums = tree(extras)
    mass = jnp.sum(sums[1:2, :], axis=1, keepdims=True)
    if not early:
        outs[1][...] = sums
    end = jnp.where(odd == 0, layers - 1, 0)
    arrive = jnp.where(lax.axis_index("layer") == end, 0.0, damping * spill[...].astype(F32))
    walk = damping * (1.0 - coupling)
    own = walk * (sum(walks[:2]) + mass / node_total) + (1.0 - damping)
    peer = walk * sum(walks[2:])
    part[0, 0:blocks, :] = arrive[0:blocks] + jnp.where(odd == 0, own, peer)
    part[0, blocks:, :] = arrive[blocks:] + jnp.where(odd == 0, peer, own)


def closing(xold, *rest):
    shared, (xnew, change) = rest[:-2], rest[-2:]
    x = joined(shared)
    xnew[...] = x
    change[...] = jnp.broadcast_to(lane_sum(jnp.abs(x - xold[...])), change.shape)


def flatten(xnew, ranks):
    wide = xnew.shape[1] // 128
    blocks = ranks.shape[0] // wide
    start = pl.multiple_of(lax.axis_index("row") * blocks, blocks)
    own = xnew[pl.ds(start, blocks), :]
    for w in range(wide):
        ranks[pl.ds(w, blocks, wide), :] = own[:, w * 128 : (w + 1) * 128]


def totals(*refs):
    early, late, out = refs[: ITERS - 1], refs[ITERS - 1 : -1], refs[-1]
    rows = [ref[2:3, :] for ref in early] + [tree([ref[0:1, :] for ref in late])]
    for t, row in enumerate(rows):
        out[0:1, t : t + 1] = jnp.sum(row, axis=1, keepdims=True)


def to_others(x):
    rows, cols = lax.axis_size("row"), lax.axis_size("col")
    got = []
    for step in range(1, cols):
        pairs = []
        for row in range(rows):
            for col in range(cols):
                other = (col + step) % cols if cols & (cols - 1) else col ^ step
                pairs.append((row * cols + col, (row ^ (step > 1)) * cols + other))
        got.append(lax.ppermute(x, ("row", "col"), pairs))
    return got


def to_rows(x):
    rows = lax.axis_size("row")
    if rows == 2:
        return x, lax.ppermute(x, "row", [(0, 1), (1, 0)])
    return (lax.all_gather(x, "row", axis=0, tiled=True),)


def to_layers(spill):
    layers, rows = lax.axis_size("layer"), lax.axis_size("row")
    pairs = []
    for layer in range(layers):
        for row in range(rows):
            other = layer + 1 if row % 2 == 1 else layer - 1
            here = layer * rows + row
            pairs.append((here, other * rows + row if 0 <= other < layers else layer * rows + (row ^ 1)))
    return lax.ppermute(spill, ("layer", "row"), pairs)


def local(block_values, block_rows, block_cols, block_count, dangling, start_ranks):
    slots, edge = block_values.shape[3], block_values.shape[-1]
    span = start_ranks.shape[-1]
    row_devices = lax.axis_size("row")
    layers = lax.axis_size("layer")
    node_total = row_devices * lax.axis_size("col") * span
    blocks = span // edge
    col_blk = row_devices * blocks
    flat = (span // 128, 128)
    arguments = [
        block_values.reshape(slots, edge, edge), block_cols.reshape(1, slots),
        block_rows.reshape(1, slots), block_count.reshape(1, 1), start_ranks.reshape(flat),
        dangling.reshape(flat),
    ]
    arguments = [
        x if x.size == 1 else pltpu.with_memory_space_constraint(x, pltpu.HBM) for x in arguments
    ]

    def shape(n, dtype=F32):
        return jax.ShapeDtypeStruct((n, edge), dtype)

    def lead(n):
        return jax.ShapeDtypeStruct((1, n, edge), F32)

    packed, values, pick, marks = call(
        opening,
        (lead(slots + META + 2 * blocks), pltpu.VMEM((slots, edge, edge), BF16),
         pltpu.VMEM((slots, col_blk), BF16), pltpu.VMEM((META, LANES), F32)),
        (HBM, HBM, HBM, pl.BlockSpec(memory_space=pl.ANY), HBM, HBM),
        [pltpu.VMEM((1, slots), jnp.int32),
         pltpu.VMEM((1, slots), jnp.int32), pltpu.VMEM((1, 1), jnp.int32), pltpu.VMEM(flat, F32),
         pltpu.VMEM(flat, jnp.int32), pltpu.SemaphoreType.DMA((5 + CHUNKS,))],
    )(*arguments)
    shared = to_rows(packed)
    turned = call(turn, pltpu.VMEM((slots, edge, edge), BF16), (VMEM,))(values)
    lanes = jax.ShapeDtypeStruct((META, LANES), F32)
    products = jax.ShapeDtypeStruct((slots * edge // LANES + META, LANES), F32)
    sent = (products, shape(2 * blocks, BF16), shape(col_blk))
    payload, spill, x, inv, kinv = call(
        functools.partial(first, layers), sent + (shape(col_blk), shape(col_blk)),
        (VMEM,) * (3 + len(shared)),
    )(turned, pick, marks, *shared)
    changes = []
    for t in range(ITERS):
        if t:
            payload, spill, x = call(
                functools.partial(middle, layers), sent, (VMEM,) * (6 + len(shared)),
            )(turned, pick, marks, inv, kinv, x, *shared)
        arriving = to_layers(spill)
        others = to_others(payload)
        part, *change = call(
            functools.partial(partial, layers, node_total, t == 0),
            (lead(2 * blocks), lanes)[: 1 + (t > 0)], (VMEM,) * (2 + len(others)),
        )(arriving, payload, *others)
        changes += change
        shared = to_rows(part)
    xnew, last = call(closing, (shape(col_blk), lanes), (VMEM,) * (1 + len(shared)))(x, *shared)
    lates = [last] + to_others(last)
    ranks = call(flatten, jax.ShapeDtypeStruct(flat, F32), (VMEM,))(xnew)
    residuals = call(
        totals, jax.ShapeDtypeStruct((1, ITERS), F32),
        (VMEM,) * (ITERS - 1 + len(lates)),
    )(*changes, *lates)
    return ranks.reshape(start_ranks.shape), residuals.reshape(ITERS, 1)


def solution(mesh):
    placed = (
        P("layer", "row", "col", None, None, None),
        P("layer", "row", "col", None),
        P("layer", "row", "col", None),
        P("layer", "row", "col"),
        P("layer", "row", "col", None),
        P("layer", "row", "col", None),
    )
    return jax.shard_map(
        local,
        mesh=mesh,
        in_specs=placed,
        out_specs=(P("layer", "row", "col", None), P(None, "layer")),
        check_vma=False,
    )
```

```python
import functools
import jax
import jax.numpy as jnp
from jax import lax
from jax.experimental import pallas as pl
from jax.experimental.pallas import tpu as pltpu
from jax.sharding import PartitionSpec as P

ITERS = 3
damping = 0.85
coupling = 0.3

F32 = jnp.float32
BF16 = jnp.bfloat16
VMEM = pl.BlockSpec(memory_space=pltpu.VMEM)
HBM = pl.BlockSpec(memory_space=pltpu.HBM)
META = 8
LANES = 128
CHUNKS = 4


def call(body, outs, specs, scratch=(), aliases={}):
    return pl.pallas_call(
        body,
        out_shape=outs,
        in_specs=specs,
        out_specs=(VMEM,) * len(outs) if isinstance(outs, tuple) else VMEM,
        scratch_shapes=scratch,
        input_output_aliases=aliases,
        compiler_params=pltpu.CompilerParams(vmem_limit_bytes=24 * 1024 * 1024),
    )


def two_terms(x):
    hi = x.astype(BF16)
    return hi, (x - hi.astype(F32)).astype(BF16)


def place(onehot, rows):
    hi, lo = two_terms(rows)
    return jnp.dot(onehot, hi, preferred_element_type=F32) + jnp.dot(
        onehot, lo, preferred_element_type=F32
    )


def tree(terms):
    while len(terms) > 1:
        terms = [sum(terms[k + 1 : k + 2], terms[k]) for k in range(0, len(terms), 2)]
    return terms[0]


def to_blocks(ref, edge):
    wide = edge // 128
    count = ref.shape[0] // wide
    return jnp.concatenate([ref[pl.ds(w, count, wide), :] for w in range(wide)], axis=1)


def opening(values_h, cols_h, rows_h, count_h, x_h, dangling_h, packed, values, pick, marks,
            cols, rows, count, x, dangling, sems):
    slots, edge, _ = values.shape
    blocks = x.shape[0] * 128 // edge
    step = slots // CHUNKS
    large = [
        pltpu.make_async_copy(
            values_h.at[pl.ds(k * step, step)], values.at[pl.ds(k * step, step)], sems.at[k]
        )
        for k in range(CHUNKS)
    ]
    pairs = ((cols_h, cols), (rows_h, rows), (count_h, count), (x_h, x), (dangling_h, dangling))
    small = [
        pltpu.make_async_copy(source, target, sems.at[CHUNKS + k])
        for k, (source, target) in enumerate(pairs)
    ]
    for copy in small + large:
        copy.start()
    for copy in small:
        copy.wait()
    live = lax.broadcasted_iota(jnp.int32, (1, slots), 1) < count[...]
    packed[0, slots : slots + META, :] = jnp.zeros((META, edge), F32)
    packed[0, slots : slots + 1, 0:slots] = jnp.where(live, cols[...], -1).astype(F32)
    marks[...] = jnp.zeros((META, LANES), F32)
    marks[0:1, 0:slots] = jnp.where(live, rows[...], -1).astype(F32)
    source_ids = lax.broadcasted_iota(jnp.int32, (pick.shape[1], slots), 0)
    pick[...] = (source_ids == cols[...]).astype(F32).T.astype(BF16)
    at = slots + META
    packed[0, at : at + blocks, :] = to_blocks(x, edge)
    packed[0, at + blocks : at + 2 * blocks, :] = 1.0 - to_blocks(dangling, edge).astype(F32)
    ones = jnp.ones((16, edge), BF16)
    for k in range(CHUNKS):
        large[k].wait()
        for s in range(k * step, (k + 1) * step):
            block = values[s]
            got = jnp.dot(ones, block, preferred_element_type=F32)
            packed[0, s : s + 1, :] = got[0:1, :]


def turn(values, turned):
    for s in range(values.shape[0]):
        turned[s] = values[s].T


def send_out(layers, pair_rows, x, inv, kinv, turned, pick, marks, payload, spill, xcur):
    slots, wide = turned.shape[0], turned.shape[1] // LANES
    scaled = (x * kinv).astype(BF16)
    picked = jnp.dot(pick[...], scaled, preferred_element_type=F32).astype(BF16)
    group = 16
    for g in range(slots // group):
        lhs = picked[g * group : (g + 1) * group, :]
        for k in range(group):
            s = g * group + k
            got = jnp.dot(lhs, turned[s], preferred_element_type=F32)
            for w in range(wide):
                at = w * slots + s
                payload[at : at + 1, :] = got[k : k + 1, w * LANES : (w + 1) * LANES]
    meta = wide * slots
    payload[meta : meta + META, :] = marks[...]
    payload[meta + 1 : meta + 2, :] = lane_sum(x * inv)
    layer = lax.axis_index("layer")
    spread = jnp.where((layer == 0) | (layer == layers - 1), 1.0, 0.5).astype(F32) * coupling
    if x.shape[0] == pair_rows:
        own = x
    else:
        first_row = pl.multiple_of((lax.axis_index("row") // 2) * pair_rows, pair_rows)
        own = xcur[pl.ds(first_row, pair_rows), :]
    spill[...] = (own * spread).astype(BF16)


def first(layers, turned, pick, marks, *rest):
    shared, (payload, spill, xcur, inv_o, kinv_o) = rest[:-5], rest[-5:]
    slots = turned.shape[0]
    at = slots + META
    blocks = (shared[0].shape[1] - at) // 2
    if len(shared) == 1:
        parts = [(shared[0].at[r], r * blocks) for r in range(shared[0].shape[0])]
    else:
        row = lax.axis_index("row")
        starts = (row * blocks, (1 - row) * blocks)
        parts = [(ref.at[0], pl.multiple_of(at, blocks)) for ref, at in zip(shared, starts)]
    degree = None
    block_ids = lax.broadcasted_iota(jnp.int32, (xcur.shape[0], slots), 0).astype(F32)
    for ref, start in parts:
        onehot = (block_ids == ref[slots : slots + 1, 0:slots]).astype(BF16)
        part = place(onehot, ref[0:slots, :])
        degree = part if degree is None else degree + part
        mine = pl.ds(start, blocks)
        xcur[mine, :] = ref[at : at + blocks, :]
        kinv_o[mine, :] = ref[at + blocks : at + 2 * blocks, :]
    x, keep = xcur[...], kinv_o[...]
    inv = 1.0 / (keep * degree + 1.0)
    kinv = keep * inv
    inv_o[...] = inv
    kinv_o[...] = kinv
    send_out(layers, 2 * blocks, x, inv, kinv, turned, pick, marks, payload, spill, xcur)


def joined(parts):
    parts = [ref[k] for ref in parts for k in range(ref.shape[0])]
    pairs = [parts[2 * k] + parts[2 * k + 1] for k in range(len(parts) // 2)]
    return pairs[0] if len(pairs) == 1 else jnp.concatenate(pairs, axis=0)


def lane_sum(x):
    row = jnp.sum(x, axis=0, keepdims=True)
    return sum(row[:, w : w + LANES] for w in range(0, row.shape[1], LANES))


def middle(layers, turned, pick, marks, inv_i, kinv_i, xold, *rest):
    shared, (payload, spill, xcur) = rest[:-3], rest[-3:]
    x = joined(shared)
    xcur[...] = x
    send_out(layers, shared[0].shape[1], x, inv_i[...], kinv_i[...], turned, pick, marks, payload,
             spill, xcur)
    meta = payload.shape[0] - META
    payload[meta + 2 : meta + 3, :] = lane_sum(jnp.abs(x - xold[...]))


def partial(layers, node_total, early, spill, *rest):
    pays, outs = (rest[:-1], rest[-1:]) if early else (rest[:-2], rest[-2:])
    part = outs[0]
    meta, wide = pays[0].shape[0] - META, part.shape[2] // LANES
    slots = meta // wide
    blocks = part.shape[1] // 2
    odd = lax.axis_index("row") % 2
    first_block = (lax.axis_index("col") * blocks).astype(F32)
    block_ids = lax.broadcasted_iota(jnp.int32, (blocks, slots), 0).astype(F32) + first_block
    walks, extras = [], []
    for pay in pays:
        onehot = (block_ids == pay[meta : meta + 1, 0:slots]).astype(BF16)
        terms = [pay[w * slots : (w + 1) * slots, :] for w in range(wide)]
        walks.append(place(onehot, jnp.concatenate(terms, axis=1)))
        extras.append(pay[meta : meta + META, :])
    sums = tree(extras)
    mass = jnp.sum(sums[1:2, :], axis=1, keepdims=True)
    if not early:
        outs[1][...] = sums
    end = jnp.where(odd == 0, layers - 1, 0)
    arrive = jnp.where(lax.axis_index("layer") == end, 0.0, damping * spill[...].astype(F32))
    walk = damping * (1.0 - coupling)
    own = walk * (walks[0] + sum(walks[1::2]) + mass / node_total) + (1.0 - damping)
    peer = walk * sum(walks[2::2])
    part[0, 0:blocks, :] = arrive[0:blocks] + jnp.where(odd == 0, own, peer)
    part[0, blocks:, :] = arrive[blocks:] + jnp.where(odd == 0, peer, own)


def closing(xold, *rest):
    shared, (xnew, change) = rest[:-2], rest[-2:]
    x = joined(shared)
    xnew[...] = x
    change[...] = jnp.broadcast_to(lane_sum(jnp.abs(x - xold[...])), change.shape)


def flatten(xnew, ranks):
    wide = xnew.shape[1] // 128
    blocks = ranks.shape[0] // wide
    start = pl.multiple_of(lax.axis_index("row") * blocks, blocks)
    own = xnew[pl.ds(start, blocks), :]
    for w in range(wide):
        ranks[pl.ds(w, blocks, wide), :] = own[:, w * 128 : (w + 1) * 128]


def totals(*refs):
    early, late, out = refs[: ITERS - 1], refs[ITERS - 1 : -1], refs[-1]
    rows = [ref[2:3, :] for ref in early] + [tree([ref[0:1, :] for ref in late])]
    for t, row in enumerate(rows):
        out[0:1, t : t + 1] = jnp.sum(row, axis=1, keepdims=True)


def to_others(x):
    rows, cols = lax.axis_size("row"), lax.axis_size("col")
    got = []
    for step in range(1, cols):
        pairs = []
        for row in range(rows):
            for col in range(cols):
                other = (col + step) % cols if cols & (cols - 1) else col ^ step
                pairs.append((row * cols + col, (row ^ (step % 2 == 0)) * cols + other))
        got.append(lax.ppermute(x, ("row", "col"), pairs))
    return got


def to_rows(x):
    rows = lax.axis_size("row")
    if rows == 2:
        return x, lax.ppermute(x, "row", [(0, 1), (1, 0)])
    return (lax.all_gather(x, "row", axis=0, tiled=True),)


def to_layers(spill):
    layers, rows = lax.axis_size("layer"), lax.axis_size("row")
    pairs = []
    for layer in range(layers):
        for row in range(rows):
            other = layer + 1 if row % 2 == 1 else layer - 1
            here = layer * rows + row
            pairs.append((here, other * rows + row if 0 <= other < layers else layer * rows + (row ^ 1)))
    return lax.ppermute(spill, ("layer", "row"), pairs)


def local(block_values, block_rows, block_cols, block_count, dangling, start_ranks):
    slots, edge = block_values.shape[3], block_values.shape[-1]
    span = start_ranks.shape[-1]
    row_devices = lax.axis_size("row")
    layers = lax.axis_size("layer")
    node_total = row_devices * lax.axis_size("col") * span
    blocks = span // edge
    col_blk = row_devices * blocks
    flat = (span // 128, 128)
    arguments = [
        block_values.reshape(slots, edge, edge), block_cols.reshape(1, slots),
        block_rows.reshape(1, slots), block_count.reshape(1, 1), start_ranks.reshape(flat),
        dangling.reshape(flat),
    ]
    arguments = [
        x if x.size == 1 else pltpu.with_memory_space_constraint(x, pltpu.HBM) for x in arguments
    ]

    def shape(n, dtype=F32):
        return jax.ShapeDtypeStruct((n, edge), dtype)

    def lead(n):
        return jax.ShapeDtypeStruct((1, n, edge), F32)

    packed, values, pick, marks = call(
        opening,
        (lead(slots + META + 2 * blocks), pltpu.VMEM((slots, edge, edge), BF16),
         pltpu.VMEM((slots, col_blk), BF16), pltpu.VMEM((META, LANES), F32)),
        (HBM, HBM, HBM, pl.BlockSpec(memory_space=pl.ANY), HBM, HBM),
        [pltpu.VMEM((1, slots), jnp.int32),
         pltpu.VMEM((1, slots), jnp.int32), pltpu.VMEM((1, 1), jnp.int32), pltpu.VMEM(flat, F32),
         pltpu.VMEM(flat, jnp.int32), pltpu.SemaphoreType.DMA((5 + CHUNKS,))],
    )(*arguments)
    shared = to_rows(packed)
    turned = call(turn, pltpu.VMEM((slots, edge, edge), BF16), (VMEM,))(values)
    lanes = jax.ShapeDtypeStruct((META, LANES), F32)
    products = jax.ShapeDtypeStruct((slots * edge // LANES + META, LANES), F32)
    sent = (products, shape(2 * blocks, BF16), shape(col_blk))
    payload, spill, x, inv, kinv = call(
        functools.partial(first, layers), sent + (shape(col_blk), shape(col_blk)),
        (VMEM,) * (3 + len(shared)),
    )(turned, pick, marks, *shared)
    changes = []
    for t in range(ITERS):
        if t:
            payload, spill, x = call(
                functools.partial(middle, layers), sent, (VMEM,) * (6 + len(shared)),
            )(turned, pick, marks, inv, kinv, x, *shared)
        arriving = to_layers(spill)
        others = to_others(payload)
        part, *change = call(
            functools.partial(partial, layers, node_total, t == 0),
            (lead(2 * blocks), lanes)[: 1 + (t > 0)], (VMEM,) * (2 + len(others)),
        )(arriving, payload, *others)
        changes += change
        shared = to_rows(part)
    xnew, last = call(closing, (shape(col_blk), lanes), (VMEM,) * (1 + len(shared)))(x, *shared)
    lates = [last] + to_others(last)
    ranks = call(flatten, jax.ShapeDtypeStruct(flat, F32), (VMEM,))(xnew)
    residuals = call(
        totals, jax.ShapeDtypeStruct((1, ITERS), F32),
        (VMEM,) * (ITERS - 1 + len(lates)),
    )(*changes, *lates)
    return ranks.reshape(start_ranks.shape), residuals.reshape(ITERS, 1)


def solution(mesh):
    placed = (
        P("layer", "row", "col", None, None, None),
        P("layer", "row", "col", None),
        P("layer", "row", "col", None),
        P("layer", "row", "col"),
        P("layer", "row", "col", None),
        P("layer", "row", "col", None),
    )
    return jax.shard_map(
        local,
        mesh=mesh,
        in_specs=placed,
        out_specs=(P("layer", "row", "col", None), P(None, "layer")),
        check_vma=False,
    )
```
